256 devices in a mesh: groups: 4 (over y, x), dp: 2 (over core), seq: 32 (over z).
Axes of the slice: x: 2, y: 2, z: 32, core: 2. Of those that a mesh axis runs over, the one named last changes fastest.
The devices are a block of a 4x8x32 slice.
Arguments:
- history: bfloat16 [16, 3072, 1024], P(('groups', 'dp'), 'seq'), parts along dimension 0, may hold values from -20 to 20
- candidates: bfloat16 [8, 2048, 1024], P(('groups', 'dp'), 'seq'), parts along dimension 0, may hold values from -6 to 6
- lengths: int32 [16], P(('groups', 'dp')), parts along dimension 0, may hold values from 384 to 3072
- assignment: int32 [8, 2048], P(('groups', 'dp'), 'seq'), parts along dimension 0, may hold values from 0 to 1, as said below
- weight_in: bfloat16 [1024, 4096], replicated, may hold values from -0.1875 to 0.1875
- weight_out: bfloat16 [1024, 1024], replicated, may hold values from -0.1875 to 0.1875
- gain_in: float32 [1024], replicated, may hold values from 0.25 to 1.75
- gain_attn: float32 [1024], replicated, may hold values from 0.25 to 1.75
Outputs:
- history_out: bfloat16 [16, 3072, 1024], P(('groups', 'dp'), 'seq'), parts along dimension 0
- candidate_out: bfloat16 [8, 2048, 1024], P(('groups', 'dp'), 'seq'), parts along dimension 0
The draws below stay inside these ranges and needn't reach their ends.
There are 4 independent parts, one for each index of `groups`. The reference program is written for one: setup_inputs(seed, part) draws one part's arguments, and reference() takes and returns one part's arrays. A program takes and returns all parts, laid end to end along the dimension named above; an argument that names none is the same for every part. Nothing has to cross between parts.
Inputs may be any that keep to these rules, and one draw needn't show every extreme that they name: `assignment`: of the 64 candidates of one device, at most 40 belong to either history; in every dp index some device has exactly 40 of the first and another exactly 40 of the second.
All inputs are finite; a program needn't handle non-finite values.
Results may differ from the reference program's by a relative error of at most 0.0075.
Values may be sent and summed in bfloat16 or wider, within the bound.
No kernel may reach another device: no remote copies, remote signals or barrier semaphores. Data moves between devices by JAX's collectives and lax.ppermute only.
A program may use at most 192 MiB of HBM per device.

```python
import math
import jax
import jax.numpy as jnp
from jax import lax

D = 1024
H = 16
HD = 64
HIST_DP = 2
CAND_DEV = 64
LENGTH = 3072
CAP = 40
HISTS = 4
CS = 2048
N_DP = 2
N_SEQ = 32


def draw_history(key, part):
    first_key = jax.random.fold_in(key, 11)
    base = jnp.clip(jax.random.normal(first_key, (HISTS, LENGTH, D), jnp.float32), -4.0, 4.0)
    return base.astype(jnp.bfloat16)


def draw_assignment(key, part):
    count_key = jax.random.fold_in(key, 21)
    full_key = jax.random.fold_in(key, 22)
    other_key = jax.random.fold_in(key, 23)
    order_key = jax.random.fold_in(key, 24)
    counts = jax.random.randint(count_key, (N_DP, N_SEQ), CAND_DEV - CAP, CAP + 1)
    full_block = jax.random.randint(full_key, (N_DP, 1), 0, N_SEQ)
    other_block = (full_block + 1 + jax.random.randint(other_key, (N_DP, 1), 0, N_SEQ - 1)) % N_SEQ
    blocks = jnp.arange(N_SEQ, dtype=jnp.int32)[None, :]
    counts = jnp.where(blocks == full_block, CAP, counts)
    counts = jnp.where(blocks == other_block, CAND_DEV - CAP, counts)
    row_keys = jax.random.split(order_key, N_DP * N_SEQ)
    ranks = jax.vmap(lambda one_key: jax.random.permutation(one_key, jnp.arange(CAND_DEV, dtype=jnp.int32)))(row_keys)
    ranks = ranks.reshape(N_DP, N_SEQ, CAND_DEV)
    chosen = (ranks >= counts[:, :, None]).astype(jnp.int32)
    return chosen.reshape(N_DP, CS)


def touch_ends(array, own_key, low, top_value):
    place = [jax.random.randint(jax.random.fold_in(own_key, axis), (), 0, length) for axis, length in enumerate(array.shape)]
    main_axis = array.shape.index(max(array.shape))
    neighbour = place[:main_axis] + [(place[main_axis] + 1) % array.shape[main_axis]] + place[main_axis + 1:]
    return array.at[tuple(place)].set(low).at[tuple(neighbour)].set(top_value)


def block_levels(rng, dims, pieces, low, largest):
    level = 1.0
    for dim, blocks in pieces:
        heights = jax.random.uniform(jax.random.fold_in(jax.random.fold_in(rng, 6), dim), (blocks,), jnp.float32, low / len(pieces), largest / len(pieces))
        level = level * jnp.repeat(jnp.exp(heights), dims[dim] // blocks).reshape((-1,) + (1,) * (len(dims) - 1 - dim))
    return level


def normal_values(own_key, dims, width, limit, cuts=(), kind=jnp.bfloat16):
    entries = jax.random.normal(own_key, dims, jnp.float32) * width
    if len(cuts) > 0:
        entries = block_levels(own_key, dims, cuts, -0.22, 0.18) * entries
    return jnp.clip(entries, min=-limit, max=limit).astype(kind)


def setup_inputs(seed: int = 0, part: int = 0) -> dict:
    seeds = jax.random.split(jax.random.key(seed), 9)
    part_splits = jax.random.split(jax.random.fold_in(seeds[8], part), 9)
    history = draw_history(jax.random.fold_in(jax.random.fold_in(seeds[8], part), 71), part)
    candidates = normal_values(part_splits[1], (N_DP, CS, D), 1.0, 6.0, ((0, 2), (1, 32)))
    lengths = touch_ends(jax.random.randint(part_splits[2], (HISTS,), LENGTH // 8, LENGTH + 1), jax.random.fold_in(part_splits[2], 1), LENGTH // 8, LENGTH).astype(jnp.int32)
    assignment = draw_assignment(jax.random.fold_in(jax.random.fold_in(seeds[8], part), 71), part)
    weight_in = normal_values(seeds[4], (D, 4 * D), D ** -0.5, 0.1875)
    weight_out = normal_values(seeds[5], (D, D), D ** -0.5, 0.1875)
    gain_in = jnp.clip(1.0 + 0.15 * jax.random.normal(seeds[6], (D,), jnp.float32), 0.25, 1.75)
    gain_attn = jnp.clip(1.0 + 0.15 * jax.random.normal(seeds[7], (D,), jnp.float32), 0.25, 1.75)
    return {"history": history, "candidates": candidates, "lengths": lengths, "assignment": assignment, "weight_in": weight_in, "weight_out": weight_out, "gain_in": gain_in, "gain_attn": gain_attn}


def rms_apply(values, gain):
    return values * lax.rsqrt(lax.optimization_barrier(jnp.mean(values * values, axis=-1, keepdims=True)) + 1e-06) * gain

def self_history(packed):
    query, keys, values, valid = packed
    score_scale = HD ** (-0.5)
    scores = jnp.einsum('ihe,jhe->hij', query.astype(jnp.float32), keys.astype(jnp.float32)) * score_scale
    positions = jnp.arange(LENGTH, dtype=jnp.int32)
    allowed = (positions[None, :] <= positions[:, None]) & (positions[None, :] < valid)
    weights = jnp.where(allowed[None], jax.nn.silu(scores), 0.0).astype(jnp.bfloat16)
    result = jnp.einsum('hij,jhe->ihe', weights.astype(jnp.float32), values.astype(jnp.float32))
    return result.astype(jnp.bfloat16).reshape(LENGTH, D)

def reference(history, candidates, lengths, assignment, weight_in, weight_out, gain_in, gain_attn):
    score_scale = HD ** (-0.5)
    hist_float = history.astype(jnp.float32)
    normed = rms_apply(hist_float, gain_in).astype(jnp.bfloat16).reshape(HISTS * LENGTH, D)
    projected = jnp.dot(normed, weight_in, preferred_element_type=jnp.float32)
    gate = jax.nn.silu(projected[:, :D]).astype(jnp.bfloat16)
    query = projected[:, D:2 * D].astype(jnp.bfloat16).reshape(HISTS, LENGTH, H, HD)
    keys = projected[:, 2 * D:3 * D].astype(jnp.bfloat16).reshape(HISTS, LENGTH, H, HD)
    values = projected[:, 3 * D:].astype(jnp.bfloat16).reshape(HISTS, LENGTH, H, HD)
    attended = lax.map(self_history, (query, keys, values, lengths))
    attended = attended.reshape(HISTS * LENGTH, D).astype(jnp.float32)
    gated_rows = (rms_apply(attended, gain_attn) * gate.astype(jnp.float32)).astype(jnp.bfloat16)
    history_out = (hist_float.reshape(HISTS * LENGTH, D) + jnp.dot(gated_rows, weight_out, preferred_element_type=jnp.float32)).astype(jnp.bfloat16)
    history_out = history_out.reshape(HISTS, LENGTH, D)
    cand_float = candidates.astype(jnp.float32)
    cand_normed = rms_apply(cand_float, gain_in).astype(jnp.bfloat16).reshape(N_DP * CS, D)
    cand_proj = jnp.dot(cand_normed, weight_in[:, :2 * D], preferred_element_type=jnp.float32)
    cand_gate = jax.nn.silu(cand_proj[:, :D]).astype(jnp.bfloat16)
    cand_query = cand_proj[:, D:].astype(jnp.bfloat16).reshape(N_DP, CS, H, HD)
    block_rows = math.gcd(CS, 1024)
    positions = jnp.arange(LENGTH, dtype=jnp.int32)
    outputs = []
    for dp_index in range(N_DP):
        keys_here = keys[dp_index * HIST_DP:(dp_index + 1) * HIST_DP].astype(jnp.float32)
        values_here = values[dp_index * HIST_DP:(dp_index + 1) * HIST_DP].astype(jnp.float32)
        lengths_here = lengths[dp_index * HIST_DP:(dp_index + 1) * HIST_DP]

        def cross_block(packed):
            query_block, owner = packed
            summed = jnp.zeros((block_rows, H, HD), jnp.float32)
            for member in range(HIST_DP):
                scores = jnp.einsum('che,jhe->chj', query_block.astype(jnp.float32), keys_here[member]) * score_scale
                allowed = (positions[None, None, :] < lengths_here[member]) & (owner[:, None, None] == member)
                weights = jnp.where(allowed, jax.nn.silu(scores), 0.0).astype(jnp.bfloat16)
                summed = summed + jnp.einsum('chj,jhe->che', weights.astype(jnp.float32), values_here[member])
            return summed.astype(jnp.bfloat16)
        blocks = lax.map(cross_block, (cand_query[dp_index].reshape(CS // block_rows, block_rows, H, HD), assignment[dp_index].reshape(CS // block_rows, block_rows)))
        outputs.append(blocks.reshape(CS, D))
    cross_attended = jnp.stack(outputs).reshape(N_DP * CS, D).astype(jnp.float32)
    cand_gated = (rms_apply(cross_attended, gain_attn) * cand_gate.astype(jnp.float32)).astype(jnp.bfloat16)
    candidate_out = (cand_float.reshape(N_DP * CS, D) + jnp.dot(cand_gated, weight_out, preferred_element_type=jnp.float32)).astype(jnp.bfloat16)
    return (history_out, candidate_out.reshape(N_DP, CS, D))
```

```python
import functools

import jax
import jax.numpy as jnp
from jax import lax
from jax.experimental import pallas as pl
from jax.experimental.pallas import tpu as pltpu
from jax.sharding import PartitionSpec as P

H = 16
HD = 64
CAP = 40
LANES = 128
CAND_TOP = 24
CAND_LOW = CAP - CAND_TOP
HEADS_STEP = 4
GROUP = 8
F32 = jnp.float32
BF16 = jnp.bfloat16


def rms_apply(values, gain):
    return values * lax.rsqrt(jnp.mean(values * values, axis=-1, keepdims=True) + 1e-06) * gain


def silu(values):
    half = values * 0.5
    return half + half * jnp.tanh(half)


def swap_halves(values):
    return pltpu.roll(values, HD, 1)


def low_lanes(rows):
    return lax.broadcasted_iota(jnp.int32, (rows, LANES), 1) < HD


def join(first, second):
    return jnp.where(low_lanes(first.shape[0]), first, second)


def selection(owner_row, member):
    count = owner_row.shape[1]
    mine = (owner_row == member).astype(F32)
    before = (
        lax.broadcasted_iota(jnp.int32, (count, count), 0)
        < lax.broadcasted_iota(jnp.int32, (count, count), 1)
    ).astype(F32)
    rank = jnp.dot(jnp.broadcast_to(mine, (8, count)), before, preferred_element_type=F32)[0:1]
    rank = jnp.where(mine > 0.5, rank, -1.0)
    rows = lax.broadcasted_iota(jnp.int32, (2 * CAND_TOP, count), 0).astype(F32)
    return (rows == rank).astype(F32)


def project_kernel(
    axis,
    tok_share,
    lengths_ref,
    hist_ref,
    cand_ref,
    owner_ref,
    gain_ref,
    wg_ref,
    wq_ref,
    wk_ref,
    wv_ref,
    send_ref,
    gate_ref,
    cgate_ref,
    normed_ref,
):
    hist_rows = hist_ref.shape[0]
    hist_local = hist_rows // tok_share
    half = tok_share // 2
    first_token = lax.axis_index(axis) * tok_share

    @pl.when(pl.program_id(0) == 0)
    def _():
        gain = gain_ref[...]
        normed_ref[:hist_rows] = rms_apply(hist_ref[...].astype(F32), gain).astype(BF16)
        normed_ref[hist_rows:] = rms_apply(cand_ref[...].astype(F32), gain).astype(BF16)

    hist_normed = normed_ref[:hist_rows]
    keys = jnp.dot(hist_normed, wk_ref[...], preferred_element_type=F32)
    values = jnp.dot(hist_normed, wv_ref[...], preferred_element_type=F32)
    normed = normed_ref[...]
    query = jnp.dot(normed, wq_ref[...], preferred_element_type=F32)
    gate = silu(jnp.dot(normed, wg_ref[...], preferred_element_type=F32)).astype(BF16)
    gate_ref[...] = gate[:hist_rows]
    cgate_ref[...] = gate[hist_rows:]
    query = query.astype(BF16).astype(F32) * (0.5 * HD ** (-0.5))
    cand_query = query[hist_rows:].astype(BF16)
    for member in range(hist_local):
        rows = slice(member * tok_share, (member + 1) * tok_share)
        position = first_token + lax.broadcasted_iota(jnp.int32, (tok_share, LANES), 0)
        present = position < lengths_ref[member]
        picked = jnp.dot(
            selection(owner_ref[...], member).astype(BF16),
            cand_query,
            preferred_element_type=F32,
        )
        for pair in range(HEADS_STEP // 2):
            lanes = slice(pair * LANES, (pair + 1) * LANES)
            key_slab = jnp.where(present, keys[rows, lanes], 0.0)
            value_slab, query_slab = values[rows, lanes], query[rows, lanes]
            cand_slab = picked[:, lanes]
            even, odd = 2 * pair, 2 * pair + 1
            send_ref[member, even, :tok_share] = join(key_slab, swap_halves(value_slab)).astype(BF16)
            send_ref[member, odd, :tok_share] = join(swap_halves(key_slab), value_slab).astype(BF16)
            top, low = query_slab[:half], query_slab[half:]
            place = slice(tok_share, tok_share + half)
            send_ref[member, even, place] = join(top, swap_halves(low)).astype(BF16)
            send_ref[member, odd, place] = join(swap_halves(top), low).astype(BF16)
            top, low = cand_slab[:CAND_TOP], cand_slab[CAND_TOP:]
            place = slice(tok_share + half, tok_share + half + CAND_TOP)
            send_ref[member, even, place] = join(top, swap_halves(low)).astype(BF16)
            send_ref[member, odd, place] = join(swap_halves(top), low).astype(BF16)


def attend_kernel(tok_share, recv_ref, back_ref, vt_ref, q_ref, cq_ref, ot_ref, ct_ref):
    sources = recv_ref.shape[0]
    half = tok_share // 2
    groups = sources // GROUP
    keys_group, half_group = GROUP * tok_share, GROUP * half
    queries_group = 2 * half_group
    top_cands, low_cands = sources * CAND_TOP, sources * CAND_LOW
    cand_first = tok_share + half

    def keys_of(group):
        return recv_ref[group * GROUP : (group + 1) * GROUP, :tok_share].reshape(keys_group, LANES)

    def low_half(values):
        return jnp.where(low_lanes(values.shape[0]), values, 0.0).astype(BF16)

    for group in range(groups):
        members = slice(group * GROUP, (group + 1) * GROUP)
        vt_ref[group] = keys_of(group).T[HD:]
        packed = recv_ref[members, tok_share:cand_first].reshape(half_group, LANES).astype(F32)
        base = group * queries_group
        q_ref[base : base + half_group] = low_half(packed)
        q_ref[base + half_group : base + queries_group] = low_half(swap_halves(packed))
    packed = recv_ref[:, cand_first:].reshape(top_cands, LANES).astype(F32)
    cq_ref[:top_cands] = low_half(packed)
    packed = recv_ref[:, cand_first : cand_first + CAND_LOW].reshape(low_cands, LANES).astype(F32)
    cq_ref[top_cands:] = low_half(swap_halves(packed))

    def weigh(group, query, allowed=None):
        half_score = lax.dot_general(
            keys_of(group), query, (((1,), (1,)), ((), ())), preferred_element_type=F32
        )
        weight = half_score + half_score * jnp.tanh(half_score)
        if allowed is not None:
            weight = jnp.where(allowed, weight, 0.0)
        return jnp.dot(vt_ref[group], weight.astype(BF16), preferred_element_type=F32)

    for group in range(groups):
        part = weigh(group, cq_ref[...])
        ct_ref[...] = part if group == 0 else ct_ref[...] + part

    column = lax.broadcasted_iota(jnp.int32, (1, queries_group), 1)
    is_low = (column >= half_group).astype(jnp.int32)
    column = column - is_low * half_group
    source = jnp.zeros_like(column)
    for later in range(1, GROUP):
        source = source + (column >= later * half).astype(jnp.int32)
    position = source * half + column + is_low * half
    causal = lax.broadcasted_iota(jnp.int32, (keys_group, queries_group), 0) <= position
    for group in range(groups):
        base = group * queries_group
        own = slice(base, base + queries_group)
        part = weigh(group, q_ref[own], causal)
        ot_ref[:, own] = part if group == 0 else ot_ref[:, own] + part
        if group + 1 < groups:
            later = slice(base + queries_group, groups * queries_group)
            part = weigh(group, q_ref[later])
            ot_ref[:, later] = part if group == 0 else ot_ref[:, later] + part

    for group in range(groups):
        base = group * queries_group
        top = ot_ref[:, base : base + half_group]
        low = ot_ref[:, base + half_group : base + queries_group]
        joined = jnp.concatenate([top, low], axis=0).T.astype(BF16)
        back_ref[group * GROUP : (group + 1) * GROUP, :half] = joined.reshape(GROUP, half, LANES)
    top, low = ct_ref[:, :top_cands].T, ct_ref[:, top_cands:].T
    top = jnp.concatenate([top, jnp.zeros_like(top)], axis=1).reshape(sources, CAND_TOP, LANES)
    low = jnp.concatenate([jnp.zeros_like(low), low], axis=1).reshape(sources, CAND_LOW, LANES)
    back_ref[:, half : half + CAND_LOW] = (top[:, :CAND_LOW] + low).astype(BF16)
    back_ref[:, half + CAND_LOW :] = top[:, CAND_LOW:].astype(BF16)


def output_kernel(
    tok_share,
    back_ref,
    owner_ref,
    hist_ref,
    cand_ref,
    gate_ref,
    cgate_ref,
    gain_ref,
    weight_ref,
    hist_out_ref,
    cand_out_ref,
    rows_ref,
):
    half = tok_share // 2
    hist_rows = hist_ref.shape[0]
    hist_local = hist_rows // tok_share
    cand_rows = cand_ref.shape[0]
    cross = []
    for pair in range(H // 2):
        lanes = slice(pair * LANES, (pair + 1) * LANES)
        cross_slab = jnp.zeros((cand_rows, LANES), F32)
        for member in range(hist_local):
            base = member * tok_share
            even = back_ref[member * H + 2 * pair].astype(F32)
            odd = back_ref[member * H + 2 * pair + 1].astype(F32)
            upper = join(even, swap_halves(odd))
            lower = join(swap_halves(even), odd)
            rows_ref[base : base + half, lanes] = upper[:half]
            rows_ref[base + half : base + tok_share, lanes] = lower[:half]
            found = jnp.concatenate([upper[half:], lower[half:]], axis=0).astype(BF16)
            pick = selection(owner_ref[...], member).astype(BF16)
            cross_slab = cross_slab + lax.dot_general(
                pick, found, (((0,), (0,)), ((), ())), preferred_element_type=F32
            )
        rows_ref[hist_rows:, lanes] = cross_slab
    gain = gain_ref[...]
    attended = rows_ref[...]
    scaled = rms_apply(attended, gain)
    hist_gated = (scaled[:hist_rows] * gate_ref[...].astype(F32)).astype(BF16)
    cand_gated = (scaled[hist_rows:] * cgate_ref[...].astype(F32)).astype(BF16)
    gated = jnp.concatenate([hist_gated, cand_gated], axis=0)
    product = jnp.dot(gated, weight_ref[...], preferred_element_type=F32)
    hist_out_ref[...] = (hist_ref[...].astype(F32) + product[:hist_rows]).astype(BF16)
    cand_out_ref[...] = (cand_ref[...].astype(F32) + product[hist_rows:]).astype(BF16)


def per_device(history, candidates, lengths, assignment, weight_in, weight_out, gain_in, gain_attn):
    seq_devices = lax.axis_size("seq")
    hist_local, tok_share, width = history.shape
    cand_count = candidates.shape[1]
    half = tok_share // 2
    hist_rows = hist_local * tok_share
    items = hist_local * H
    assert items == seq_devices
    hist = history.reshape(hist_rows, width)
    cand = candidates.reshape(cand_count, width)
    gain_in = gain_in.reshape(1, width)
    gain_attn = gain_attn.reshape(1, width)
    send_rows = tok_share + half + CAND_TOP
    step_width = HEADS_STEP * HD
    steps = H // HEADS_STEP

    def whole(shape):
        return pl.BlockSpec(shape, lambda *_: (0,) * len(shape))

    def part(number):
        return pl.BlockSpec((width, step_width), lambda j: (0, number * steps + j))

    send, gate, cgate = pl.pallas_call(
        functools.partial(project_kernel, "seq", tok_share),
        grid=(steps,),
        in_specs=[
            pl.BlockSpec(memory_space=pltpu.SMEM),
            whole((hist_rows, width)),
            whole((cand_count, width)),
            whole((1, cand_count)),
            whole((1, width)),
            part(0),
            part(1),
            part(2),
            part(3),
        ],
        out_specs=[
            pl.BlockSpec((hist_local, HEADS_STEP, send_rows, LANES), lambda j: (0, j, 0, 0)),
            pl.BlockSpec((hist_rows, step_width), lambda j: (0, j)),
            pl.BlockSpec((cand_count, step_width), lambda j: (0, j)),
        ],
        out_shape=[
            jax.ShapeDtypeStruct((hist_local, H, send_rows, LANES), BF16),
            jax.ShapeDtypeStruct((hist_rows, width), BF16),
            jax.ShapeDtypeStruct((cand_count, width), BF16),
        ],
        scratch_shapes=[pltpu.VMEM((hist_rows + cand_count, width), BF16)],
        name="project",
    )(lengths, hist, cand, assignment, gain_in, weight_in, weight_in, weight_in, weight_in)
    recv = lax.all_to_all(
        send.reshape(items, send_rows, LANES), "seq", split_axis=0, concat_axis=0, tiled=True
    )
    length = seq_devices * tok_share
    back = pl.pallas_call(
        functools.partial(attend_kernel, tok_share),
        in_specs=[pl.BlockSpec(memory_space=pltpu.VMEM)],
        out_specs=pl.BlockSpec(memory_space=pltpu.VMEM),
        out_shape=jax.ShapeDtypeStruct((seq_devices, half + CAND_TOP, LANES), BF16),
        scratch_shapes=[
            pltpu.VMEM((seq_devices // GROUP, HD, GROUP * tok_share), BF16),
            pltpu.VMEM((length, LANES), BF16),
            pltpu.VMEM((seq_devices * CAP, LANES), BF16),
            pltpu.VMEM((HD, length), F32),
            pltpu.VMEM((HD, seq_devices * CAP), F32),
        ],
        name="attend",
    )(recv)
    home = lax.all_to_all(back, "seq", split_axis=0, concat_axis=0, tiled=True)
    hist_out, cand_out = pl.pallas_call(
        functools.partial(output_kernel, tok_share),
        out_shape=[
            jax.ShapeDtypeStruct((hist_rows, width), BF16),
            jax.ShapeDtypeStruct((cand_count, width), BF16),
        ],
        scratch_shapes=[pltpu.VMEM((hist_rows + cand_count, width), F32)],
        name="combine",
    )(home, assignment, hist, cand, gate, cgate, gain_attn, weight_out)
    return hist_out.reshape(history.shape), cand_out.reshape(candidates.shape)


def solution(mesh):
    in_specs = (
        P(("groups", "dp"), "seq", None),
        P(("groups", "dp"), "seq", None),
        P(("groups", "dp")),
        P(("groups", "dp"), "seq"),
        P(),
        P(),
        P(),
        P(),
    )
    out_specs = (P(("groups", "dp"), "seq", None), P(("groups", "dp"), "seq", None))
    return jax.shard_map(
        per_device, mesh=mesh, in_specs=in_specs, out_specs=out_specs, check_vma=False
    )
```

```python
import functools

import jax
import jax.numpy as jnp
from jax import lax
from jax.experimental import pallas as pl
from jax.experimental.pallas import tpu as pltpu
from jax.sharding import PartitionSpec as P

H = 16
HD = 64
CAP = 40
LANES = 128
CAND_HALF = CAP // 2
CAND_PAD = 24
HEADS_STEP = 4
PARTS = 4
VMEM_LIMIT = 28 << 20
GROUP = 8
F32 = jnp.float32
BF16 = jnp.bfloat16


def rms_apply(values, gain):
    return values * lax.rsqrt(jnp.mean(values * values, axis=-1, keepdims=True) + 1e-06) * gain


def silu(values):
    half = values * 0.5
    return half + half * jnp.tanh(half)


def swap_halves(values):
    return pltpu.roll(values, HD, 1)


def low_lanes(rows):
    return lax.broadcasted_iota(jnp.int32, (rows, LANES), 1) < HD


def join(first, second):
    return jnp.where(low_lanes(first.shape[0]), first, second)


def selection(owner_row, member):
    count = owner_row.shape[1]
    mine = (owner_row == member).astype(F32)
    before = (
        lax.broadcasted_iota(jnp.int32, (count, count), 0)
        < lax.broadcasted_iota(jnp.int32, (count, count), 1)
    ).astype(F32)
    rank = jnp.dot(jnp.broadcast_to(mine, (8, count)), before, preferred_element_type=F32)[0:1]
    row = jnp.where(rank < CAND_HALF, rank, rank + (CAND_PAD - CAND_HALF))
    row = jnp.where(mine > 0.5, row, -1.0)
    rows = lax.broadcasted_iota(jnp.int32, (2 * CAND_PAD, count), 0).astype(F32)
    return (rows == row).astype(BF16)


def project_kernel(
    axis,
    tok_share,
    lengths_hbm,
    hist_hbm,
    cand_hbm,
    owner_hbm,
    gain_hbm,
    weight_hbm,
    send_ref,
    gate_ref,
    cgate_ref,
    lengths_ref,
    hist_ref,
    cand_ref,
    owner_ref,
    gain_ref,
    weight_ref,
    normed_ref,
    loaded,
    arrived,
):
    hist_rows, width = hist_ref.shape
    hist_local = hist_rows // tok_share
    half = tok_share // 2
    chunk = tok_share + half + CAND_HALF
    step_width = HEADS_STEP * HD
    steps = H // HEADS_STEP

    def fetch(step, part):
        start = part * width + step * step_width
        return pltpu.make_async_copy(
            weight_hbm.at[:, start : start + step_width],
            weight_ref.at[step, part],
            arrived.at[step, part],
        )

    loads = [
        pltpu.make_async_copy(source, target, loaded.at[number])
        for number, (source, target) in enumerate(
            (
                (gain_hbm, gain_ref),
                (hist_hbm, hist_ref),
                (cand_hbm, cand_ref),
                (owner_hbm, owner_ref),
                (lengths_hbm, lengths_ref),
            )
        )
    ]
    for load in loads:
        load.start()
    for step in range(steps):
        for part in (2, 3, 1, 0):
            fetch(step, part).start()
    for load in loads:
        load.wait()
    gain = gain_ref[...]
    normed_ref[:hist_rows] = rms_apply(hist_ref[...].astype(F32), gain).astype(BF16)
    normed_ref[hist_rows:] = rms_apply(cand_ref[...].astype(F32), gain).astype(BF16)
    picks = [selection(owner_ref[...], member) for member in range(hist_local)]
    position = lax.axis_index(axis) * tok_share + lax.broadcasted_iota(jnp.int32, (tok_share, LANES), 0)

    for step in range(steps):

        def times(rows, part):
            fetch(step, part).wait()
            return jnp.dot(normed_ref[:rows], weight_ref[step, part], preferred_element_type=F32)

        all_rows = normed_ref.shape[0]
        keys = times(hist_rows, 2)
        values = times(hist_rows, 3)
        query = times(all_rows, 1).astype(BF16).astype(F32) * (0.5 * HD ** (-0.5))
        cand_query = query[hist_rows:].astype(BF16)
        for member in range(hist_local):
            rows = slice(member * tok_share, (member + 1) * tok_share)
            picked = jnp.dot(picks[member], cand_query, preferred_element_type=F32)
            present = position < lengths_ref[member]
            for pair in range(HEADS_STEP // 2):
                lanes = slice(pair * LANES, (pair + 1) * LANES)
                key_slab = jnp.where(present, keys[rows, lanes], 0.0)
                value_slab, query_slab, cand_slab = values[rows, lanes], query[rows, lanes], picked[:, lanes]
                even = (member * H + step * HEADS_STEP + 2 * pair) * chunk
                odd = even + chunk
                send_ref[even : even + tok_share] = join(key_slab, swap_halves(value_slab)).astype(BF16)
                send_ref[odd : odd + tok_share] = join(swap_halves(key_slab), value_slab).astype(BF16)
                top, low = query_slab[:half], query_slab[half:]
                even, odd = even + tok_share, odd + tok_share
                send_ref[even : even + half] = join(top, swap_halves(low)).astype(BF16)
                send_ref[odd : odd + half] = join(swap_halves(top), low).astype(BF16)
                top, low = cand_slab[:CAND_PAD], cand_slab[CAND_PAD:]
                even, odd = even + half, odd + half
                send_ref[even : even + CAND_HALF] = join(top, swap_halves(low)).astype(BF16)[:CAND_HALF]
                send_ref[odd : odd + CAND_HALF] = join(swap_halves(top), low).astype(BF16)[:CAND_HALF]
        gate = silu(times(all_rows, 0)).astype(BF16)
        columns = slice(step * step_width, (step + 1) * step_width)
        gate_ref[:, columns] = gate[:hist_rows]
        cgate_ref[:, columns] = gate[hist_rows:]


def attend_kernel(tok_share, recv_ref, back_ref, kv_ref, vt_ref, q_ref, cq_ref, ot_ref, ct_ref):
    half = tok_share // 2
    chunk, back_chunk = tok_share + half + CAND_HALF, half + CAND_HALF
    sources = recv_ref.shape[0] // chunk
    groups = sources // GROUP
    keys_group, half_group = GROUP * tok_share, GROUP * half
    queries_group = 2 * half_group
    cands = sources * CAND_HALF

    def keys_of(group):
        return kv_ref[group * keys_group : (group + 1) * keys_group]

    def low_half(values):
        return jnp.where(low_lanes(values.shape[0]), values, 0.0).astype(BF16)

    for source in range(sources):
        base = source * chunk
        kv_ref[source * tok_share : (source + 1) * tok_share] = recv_ref[base : base + tok_share]
        base = base + tok_share
        packed = recv_ref[base : base + half].astype(F32)
        place = source // GROUP * queries_group + source % GROUP * half
        q_ref[place : place + half] = low_half(packed)
        q_ref[place + half_group : place + half_group + half] = low_half(swap_halves(packed))
        base = base + half
        packed = recv_ref[base : base + CAND_HALF].astype(F32)
        place = source * CAND_HALF
        cq_ref[place : place + CAND_HALF] = low_half(packed)
        cq_ref[cands + place : cands + place + CAND_HALF] = low_half(swap_halves(packed))
    for group in range(groups):
        vt_ref[group] = keys_of(group).T[HD:]

    def weigh(group, query, allowed=None):
        half_score = lax.dot_general(
            keys_of(group), query, (((1,), (1,)), ((), ())), preferred_element_type=F32
        )
        weight = half_score + half_score * jnp.tanh(half_score)
        if allowed is not None:
            weight = jnp.where(allowed, weight, 0.0)
        return jnp.dot(vt_ref[group], weight.astype(BF16), preferred_element_type=F32)

    for group in range(groups):
        part = weigh(group, cq_ref[...])
        ct_ref[...] = part if group == 0 else ct_ref[...] + part

    column = lax.broadcasted_iota(jnp.int32, (1, queries_group), 1)
    is_low = (column >= half_group).astype(jnp.int32)
    column = column - is_low * half_group
    source = jnp.zeros_like(column)
    for later in range(1, GROUP):
        source = source + (column >= later * half).astype(jnp.int32)
    position = source * half + column + is_low * half
    causal = lax.broadcasted_iota(jnp.int32, (keys_group, queries_group), 0) <= position
    for group in range(groups):
        base = group * queries_group
        own = slice(base, base + queries_group)
        part = weigh(group, q_ref[own], causal)
        ot_ref[:, own] = part if group == 0 else ot_ref[:, own] + part
        if group + 1 < groups:
            later = slice(base + queries_group, groups * queries_group)
            part = weigh(group, q_ref[later])
            ot_ref[:, later] = part if group == 0 else ot_ref[:, later] + part

    for group in range(groups):
        base = group * queries_group
        top = ot_ref[:, base : base + half_group]
        low = ot_ref[:, base + half_group : base + queries_group]
        joined = jnp.concatenate([top, low], axis=0).T.astype(BF16)
        for member in range(GROUP):
            place = (group * GROUP + member) * back_chunk
            back_ref[place : place + half] = joined[member * half : (member + 1) * half]
    joined = jnp.concatenate([ct_ref[:, :cands], ct_ref[:, cands:]], axis=0).T.astype(BF16)
    for source in range(sources):
        place = source * back_chunk + half
        back_ref[place : place + CAND_HALF] = joined[source * CAND_HALF : (source + 1) * CAND_HALF]


def output_kernel(
    tok_share,
    back_ref,
    owner_ref,
    hist_ref,
    cand_ref,
    gate_ref,
    cgate_ref,
    gain_ref,
    weight_ref,
    hist_out_ref,
    cand_out_ref,
    rows_ref,
):
    half = tok_share // 2
    hist_rows = hist_ref.shape[0]
    hist_local = hist_rows // tok_share
    cand_rows = cand_ref.shape[0]
    chunk = half + CAND_HALF
    picks = [selection(owner_ref[...], member) for member in range(hist_local)]
    fill = jnp.zeros((CAND_PAD - CAND_HALF, LANES), F32)
    for pair in range(H // 2):
        lanes = slice(pair * LANES, (pair + 1) * LANES)
        cross_slab = jnp.zeros((cand_rows, LANES), F32)
        for member in range(hist_local):
            base = member * tok_share
            first = (member * H + 2 * pair) * chunk
            even = back_ref[first : first + half].astype(F32)
            odd = back_ref[first + chunk : first + chunk + half].astype(F32)
            rows_ref[base : base + half, lanes] = join(even, swap_halves(odd))
            rows_ref[base + half : base + tok_share, lanes] = join(swap_halves(even), odd)
            first = first + half
            even = back_ref[first : first + CAND_HALF].astype(F32)
            odd = back_ref[first + chunk : first + chunk + CAND_HALF].astype(F32)
            upper, lower = join(even, swap_halves(odd)), join(swap_halves(even), odd)
            found = jnp.concatenate([upper, fill, lower, fill], axis=0).astype(BF16)
            cross_slab = cross_slab + lax.dot_general(
                picks[member], found, (((0,), (0,)), ((), ())), preferred_element_type=F32
            )
        rows_ref[hist_rows:, lanes] = cross_slab
    gain = gain_ref[...]
    attended = rows_ref[...]
    scaled = rms_apply(attended, gain)
    hist_gated = (scaled[:hist_rows] * gate_ref[...].astype(F32)).astype(BF16)
    cand_gated = (scaled[hist_rows:] * cgate_ref[...].astype(F32)).astype(BF16)
    gated = jnp.concatenate([hist_gated, cand_gated], axis=0)
    product = jnp.dot(gated, weight_ref[...], preferred_element_type=F32)
    hist_out_ref[...] = (hist_ref[...].astype(F32) + product[:hist_rows]).astype(BF16)
    cand_out_ref[...] = (cand_ref[...].astype(F32) + product[hist_rows:]).astype(BF16)


def per_device(history, candidates, lengths, assignment, weight_in, weight_out, gain_in, gain_attn):
    seq_devices = lax.axis_size("seq")
    hist_local, tok_share, width = history.shape
    cand_count = candidates.shape[1]
    half = tok_share // 2
    hist_rows = hist_local * tok_share
    items = hist_local * H
    assert items == seq_devices
    hist = history.reshape(hist_rows, width)
    cand = candidates.reshape(cand_count, width)
    gain_in = gain_in.reshape(1, width)
    gain_attn = gain_attn.reshape(1, width)
    send_rows, back_rows = tok_share + half + CAND_HALF, half + CAND_HALF
    length = seq_devices * tok_share
    params = pltpu.CompilerParams(vmem_limit_bytes=VMEM_LIMIT)
    vmem = pl.BlockSpec(memory_space=pltpu.VMEM)

    def exchange(rows):
        pairs = rows.reshape(items, rows.shape[0] // items // 2, 2, LANES)
        moved = lax.all_to_all(pairs, "seq", split_axis=0, concat_axis=0, tiled=True)
        return pltpu.with_memory_space_constraint(moved.reshape(rows.shape), pltpu.VMEM)

    send, gate, cgate = pl.pallas_call(
        functools.partial(project_kernel, "seq", tok_share),
        in_specs=[pl.BlockSpec(memory_space=pltpu.HBM)] * 6,
        out_specs=[vmem] * 3,
        out_shape=[
            pltpu.VMEM((items * send_rows, LANES), BF16),
            jax.ShapeDtypeStruct((hist_rows, width), BF16),
            jax.ShapeDtypeStruct((cand_count, width), BF16),
        ],
        scratch_shapes=[
            pltpu.SMEM(lengths.shape, lengths.dtype),
            pltpu.VMEM(hist.shape, BF16),
            pltpu.VMEM(cand.shape, BF16),
            pltpu.VMEM(assignment.shape, assignment.dtype),
            pltpu.VMEM(gain_in.shape, F32),
            pltpu.VMEM((H // HEADS_STEP, PARTS, width, HEADS_STEP * HD), BF16),
            pltpu.VMEM((hist_rows + cand_count, width), BF16),
            pltpu.SemaphoreType.DMA((5,)),
            pltpu.SemaphoreType.DMA((H // HEADS_STEP, PARTS)),
        ],
        compiler_params=params,
        name="project",
    )(lengths, hist, cand, assignment, gain_in, weight_in)
    back = pl.pallas_call(
        functools.partial(attend_kernel, tok_share),
        in_specs=[vmem],
        out_specs=vmem,
        out_shape=pltpu.VMEM((items * back_rows, LANES), BF16),
        scratch_shapes=[
            pltpu.VMEM((length, LANES), BF16),
            pltpu.VMEM((seq_devices // GROUP, HD, GROUP * tok_share), BF16),
            pltpu.VMEM((length, LANES), BF16),
            pltpu.VMEM((seq_devices * CAP, LANES), BF16),
            pltpu.VMEM((HD, length), F32),
            pltpu.VMEM((HD, seq_devices * CAP), F32),
        ],
        compiler_params=params,
        name="attend",
    )(exchange(send))
    hist_out, cand_out = pl.pallas_call(
        functools.partial(output_kernel, tok_share),
        in_specs=[vmem] * 8,
        out_specs=[vmem] * 2,
        out_shape=[
            jax.ShapeDtypeStruct((hist_rows, width), BF16),
            jax.ShapeDtypeStruct((cand_count, width), BF16),
        ],
        scratch_shapes=[pltpu.VMEM((hist_rows + cand_count, width), F32)],
        compiler_params=params,
        name="combine",
    )(exchange(back), assignment, hist, cand, gate, cgate, gain_attn, weight_out)
    return hist_out.reshape(history.shape), cand_out.reshape(candidates.shape)


def solution(mesh):
    in_specs = (
        P(("groups", "dp"), "seq", None),
        P(("groups", "dp"), "seq", None),
        P(("groups", "dp")),
        P(("groups", "dp"), "seq"),
        P(),
        P(),
        P(),
        P(),
    )
    out_specs = (P(("groups", "dp"), "seq", None), P(("groups", "dp"), "seq", None))
    return jax.shard_map(
        per_device, mesh=mesh, in_specs=in_specs, out_specs=out_specs, check_vma=False
    )
```

```python
import functools

import jax
import jax.numpy as jnp
from jax import lax
from jax.experimental import pallas as pl
from jax.experimental.pallas import tpu as pltpu
from jax.sharding import PartitionSpec as P

H = 16
HD = 64
CAP = 40
LANES = 128
CAND_HALF = CAP // 2
CAND_PAD = 24
HEADS_STEP = 16
PARTS = 4
VMEM_LIMIT = 28 << 20
GROUP = 8
F32 = jnp.float32
BF16 = jnp.bfloat16


def rms_apply(values, gain):
    return values * lax.rsqrt(jnp.mean(values * values, axis=-1, keepdims=True) + 1e-06) * gain


def silu(values):
    half = values * 0.5
    return half + half * jnp.tanh(half)


def swap_halves(values):
    return pltpu.roll(values, HD, 1)


def low_lanes(rows):
    return lax.broadcasted_iota(jnp.int32, (rows, LANES), 1) < HD


def join(first, second):
    return jnp.where(low_lanes(first.shape[0]), first, second)


def selection(owner_row, member):
    count = owner_row.shape[1]
    mine = (owner_row == member).astype(F32)
    before = (
        lax.broadcasted_iota(jnp.int32, (count, count), 0)
        < lax.broadcasted_iota(jnp.int32, (count, count), 1)
    ).astype(F32)
    rank = jnp.dot(jnp.broadcast_to(mine, (8, count)), before, preferred_element_type=F32)[0:1]
    row = jnp.where(rank < CAND_HALF, rank, rank + (CAND_PAD - CAND_HALF))
    row = jnp.where(mine > 0.5, row, -1.0)
    rows = lax.broadcasted_iota(jnp.int32, (2 * CAND_PAD, count), 0).astype(F32)
    return (rows == row).astype(BF16)


def project_kernel(
    axis,
    tok_share,
    lengths_hbm,
    hist_hbm,
    cand_hbm,
    owner_hbm,
    gain_hbm,
    weight_hbm,
    send_ref,
    gate_ref,
    cgate_ref,
    lengths_ref,
    hist_ref,
    cand_ref,
    owner_ref,
    gain_ref,
    weight_ref,
    normed_ref,
    loaded,
    arrived,
):
    hist_rows, width = hist_ref.shape
    hist_local = hist_rows // tok_share
    half = tok_share // 2
    chunk = tok_share + half + CAND_HALF
    step_width = HEADS_STEP * HD
    steps = H // HEADS_STEP

    def fetch(step, part):
        start = part * width + step * step_width
        return pltpu.make_async_copy(
            weight_hbm.at[:, start : start + step_width],
            weight_ref.at[step, part],
            arrived.at[step, part],
        )

    loads = [
        pltpu.make_async_copy(source, target, loaded.at[number])
        for number, (source, target) in enumerate(
            (
                (gain_hbm, gain_ref),
                (hist_hbm, hist_ref),
                (cand_hbm, cand_ref),
                (owner_hbm, owner_ref),
                (lengths_hbm, lengths_ref),
            )
        )
    ]
    for load in loads:
        load.start()
    for step in range(steps):
        for part in (2, 3, 1, 0):
            fetch(step, part).start()
    for load in loads:
        load.wait()
    gain = gain_ref[...]
    normed_ref[:hist_rows] = rms_apply(hist_ref[...].astype(F32), gain).astype(BF16)
    normed_ref[hist_rows:] = rms_apply(cand_ref[...].astype(F32), gain).astype(BF16)
    picks = [selection(owner_ref[...], member) for member in range(hist_local)]
    position = lax.axis_index(axis) * tok_share + lax.broadcasted_iota(jnp.int32, (tok_share, LANES), 0)

    for step in range(steps):

        def times(rows, part):
            fetch(step, part).wait()
            return jnp.dot(normed_ref[:rows], weight_ref[step, part], preferred_element_type=F32)

        all_rows = normed_ref.shape[0]
        keys = times(hist_rows, 2)
        values = times(hist_rows, 3)
        query = times(all_rows, 1).astype(BF16).astype(F32) * (0.5 * HD ** (-0.5))
        cand_query = query[hist_rows:].astype(BF16)
        for member in range(hist_local):
            rows = slice(member * tok_share, (member + 1) * tok_share)
            picked = jnp.dot(picks[member], cand_query, preferred_element_type=F32)
            present = position < lengths_ref[member]
            for pair in range(HEADS_STEP // 2):
                lanes = slice(pair * LANES, (pair + 1) * LANES)
                key_slab = jnp.where(present, keys[rows, lanes], 0.0)
                value_slab, query_slab, cand_slab = values[rows, lanes], query[rows, lanes], picked[:, lanes]
                even = (member * H + step * HEADS_STEP + 2 * pair) * chunk
                odd = even + chunk
                send_ref[even : even + tok_share] = join(key_slab, swap_halves(value_slab)).astype(BF16)
                send_ref[odd : odd + tok_share] = join(swap_halves(key_slab), value_slab).astype(BF16)
                top, low = query_slab[:half], query_slab[half:]
                even, odd = even + tok_share, odd + tok_share
                send_ref[even : even + half] = join(top, swap_halves(low)).astype(BF16)
                send_ref[odd : odd + half] = join(swap_halves(top), low).astype(BF16)
                top, low = cand_slab[:CAND_PAD], cand_slab[CAND_PAD:]
                even, odd = even + half, odd + half
                send_ref[even : even + CAND_HALF] = join(top, swap_halves(low)).astype(BF16)[:CAND_HALF]
                send_ref[odd : odd + CAND_HALF] = join(swap_halves(top), low).astype(BF16)[:CAND_HALF]
        gate = silu(times(all_rows, 0)).astype(BF16)
        columns = slice(step * step_width, (step + 1) * step_width)
        gate_ref[:, columns] = gate[:hist_rows]
        cgate_ref[:, columns] = gate[hist_rows:]


def attend_kernel(tok_share, recv_ref, back_ref, kv_ref, vt_ref, q_ref, cq_ref, ot_ref, ct_ref):
    half = tok_share // 2
    chunk, back_chunk = tok_share + half + CAND_HALF, half + CAND_HALF
    sources = recv_ref.shape[0] // chunk
    groups = sources // GROUP
    keys_group, half_group = GROUP * tok_share, GROUP * half
    queries_group = 2 * half_group
    cands = sources * CAND_HALF

    def keys_of(group):
        return kv_ref[group * keys_group : (group + 1) * keys_group]

    def low_half(values):
        return jnp.where(low_lanes(values.shape[0]), values, 0.0).astype(BF16)

    for source in range(sources):
        base = source * chunk
        kv_ref[source * tok_share : (source + 1) * tok_share] = recv_ref[base : base + tok_share]
        base = base + tok_share
        packed = recv_ref[base : base + half].astype(F32)
        place = source // GROUP * queries_group + source % GROUP * half
        q_ref[place : place + half] = low_half(packed)
        q_ref[place + half_group : place + half_group + half] = low_half(swap_halves(packed))
        base = base + half
        packed = recv_ref[base : base + CAND_HALF].astype(F32)
        place = source * CAND_HALF
        cq_ref[place : place + CAND_HALF] = low_half(packed)
        cq_ref[cands + place : cands + place + CAND_HALF] = low_half(swap_halves(packed))
    for group in range(groups):
        vt_ref[group] = keys_of(group).T[HD:]

    def weigh(group, query, allowed=None):
        half_score = lax.dot_general(
            keys_of(group), query, (((1,), (1,)), ((), ())), preferred_element_type=F32
        )
        weight = half_score + half_score * jnp.tanh(half_score)
        if allowed is not None:
            weight = jnp.where(allowed, weight, 0.0)
        return jnp.dot(vt_ref[group], weight.astype(BF16), preferred_element_type=F32)

    for group in range(groups):
        part = weigh(group, cq_ref[...])
        ct_ref[...] = part if group == 0 else ct_ref[...] + part

    column = lax.broadcasted_iota(jnp.int32, (1, queries_group), 1)
    is_low = (column >= half_group).astype(jnp.int32)
    column = column - is_low * half_group
    source = jnp.zeros_like(column)
    for later in range(1, GROUP):
        source = source + (column >= later * half).astype(jnp.int32)
    position = source * half + column + is_low * half
    causal = lax.broadcasted_iota(jnp.int32, (keys_group, queries_group), 0) <= position
    for group in range(groups):
        base = group * queries_group
        own = slice(base, base + queries_group)
        part = weigh(group, q_ref[own], causal)
        ot_ref[:, own] = part if group == 0 else ot_ref[:, own] + part
        if group + 1 < groups:
            later = slice(base + queries_group, groups * queries_group)
            part = weigh(group, q_ref[later])
            ot_ref[:, later] = part if group == 0 else ot_ref[:, later] + part

    for group in range(groups):
        base = group * queries_group
        top = ot_ref[:, base : base + half_group]
        low = ot_ref[:, base + half_group : base + queries_group]
        joined = jnp.concatenate([top, low], axis=0).T.astype(BF16)
        for member in range(GROUP):
            place = (group * GROUP + member) * back_chunk
            back_ref[place : place + half] = joined[member * half : (member + 1) * half]
    joined = jnp.concatenate([ct_ref[:, :cands], ct_ref[:, cands:]], axis=0).T.astype(BF16)
    for source in range(sources):
        place = source * back_chunk + half
        back_ref[place : place + CAND_HALF] = joined[source * CAND_HALF : (source + 1) * CAND_HALF]


def output_kernel(
    tok_share,
    back_ref,
    owner_ref,
    hist_ref,
    cand_ref,
    gate_ref,
    cgate_ref,
    gain_ref,
    weight_ref,
    hist_out_ref,
    cand_out_ref,
    rows_ref,
):
    half = tok_share // 2
    hist_rows = hist_ref.shape[0]
    hist_local = hist_rows // tok_share
    cand_rows = cand_ref.shape[0]
    chunk = half + CAND_HALF
    picks = [selection(owner_ref[...], member) for member in range(hist_local)]
    fill = jnp.zeros((CAND_PAD - CAND_HALF, LANES), F32)
    for pair in range(H // 2):
        lanes = slice(pair * LANES, (pair + 1) * LANES)
        cross_slab = jnp.zeros((cand_rows, LANES), F32)
        for member in range(hist_local):
            base = member * tok_share
            first = (member * H + 2 * pair) * chunk
            even = back_ref[first : first + half].astype(F32)
            odd = back_ref[first + chunk : first + chunk + half].astype(F32)
            rows_ref[base : base + half, lanes] = join(even, swap_halves(odd))
            rows_ref[base + half : base + tok_share, lanes] = join(swap_halves(even), odd)
            first = first + half
            even = back_ref[first : first + CAND_HALF].astype(F32)
            odd = back_ref[first + chunk : first + chunk + CAND_HALF].astype(F32)
            upper, lower = join(even, swap_halves(odd)), join(swap_halves(even), odd)
            found = jnp.concatenate([upper, fill, lower, fill], axis=0).astype(BF16)
            cross_slab = cross_slab + lax.dot_general(
                picks[member], found, (((0,), (0,)), ((), ())), preferred_element_type=F32
            )
        rows_ref[hist_rows:, lanes] = cross_slab
    gain = gain_ref[...]
    attended = rows_ref[...]
    scaled = rms_apply(attended, gain)
    hist_gated = (scaled[:hist_rows] * gate_ref[...].astype(F32)).astype(BF16)
    cand_gated = (scaled[hist_rows:] * cgate_ref[...].astype(F32)).astype(BF16)
    gated = jnp.concatenate([hist_gated, cand_gated], axis=0)
    product = jnp.dot(gated, weight_ref[...], preferred_element_type=F32)
    hist_out_ref[...] = (hist_ref[...].astype(F32) + product[:hist_rows]).astype(BF16)
    cand_out_ref[...] = (cand_ref[...].astype(F32) + product[hist_rows:]).astype(BF16)


def per_device(history, candidates, lengths, assignment, weight_in, weight_out, gain_in, gain_attn):
    seq_devices = lax.axis_size("seq")
    hist_local, tok_share, width = history.shape
    cand_count = candidates.shape[1]
    half = tok_share // 2
    hist_rows = hist_local * tok_share
    items = hist_local * H
    assert items == seq_devices
    hist = history.reshape(hist_rows, width)
    cand = candidates.reshape(cand_count, width)
    gain_in = gain_in.reshape(1, width)
    gain_attn = gain_attn.reshape(1, width)
    send_rows, back_rows = tok_share + half + CAND_HALF, half + CAND_HALF
    length = seq_devices * tok_share
    params = pltpu.CompilerParams(vmem_limit_bytes=VMEM_LIMIT)
    vmem = pl.BlockSpec(memory_space=pltpu.VMEM)

    def exchange(rows):
        pairs = rows.reshape(items, rows.shape[0] // items // 2, 2, LANES)
        moved = lax.all_to_all(pairs, "seq", split_axis=0, concat_axis=0, tiled=True)
        return pltpu.with_memory_space_constraint(moved.reshape(rows.shape), pltpu.VMEM)

    send, gate, cgate = pl.pallas_call(
        functools.partial(project_kernel, "seq", tok_share),
        in_specs=[pl.BlockSpec(memory_space=pltpu.HBM)] * 6,
        out_specs=[vmem] * 3,
        out_shape=[
            pltpu.VMEM((items * send_rows, LANES), BF16),
            jax.ShapeDtypeStruct((hist_rows, width), BF16),
            jax.ShapeDtypeStruct((cand_count, width), BF16),
        ],
        scratch_shapes=[
            pltpu.SMEM(lengths.shape, lengths.dtype),
            pltpu.VMEM(hist.shape, BF16),
            pltpu.VMEM(cand.shape, BF16),
            pltpu.VMEM(assignment.shape, assignment.dtype),
            pltpu.VMEM(gain_in.shape, F32),
            pltpu.VMEM((H // HEADS_STEP, PARTS, width, HEADS_STEP * HD), BF16),
            pltpu.VMEM((hist_rows + cand_count, width), BF16),
            pltpu.SemaphoreType.DMA((5,)),
            pltpu.SemaphoreType.DMA((H // HEADS_STEP, PARTS)),
        ],
        compiler_params=params,
        name="project",
    )(
        *(
            pltpu.with_memory_space_constraint(argument, pltpu.HBM)
            for argument in (lengths, hist, cand, assignment, gain_in, weight_in)
        )
    )
    back = pl.pallas_call(
        functools.partial(attend_kernel, tok_share),
        in_specs=[vmem],
        out_specs=vmem,
        out_shape=pltpu.VMEM((items * back_rows, LANES), BF16),
        scratch_shapes=[
            pltpu.VMEM((length, LANES), BF16),
            pltpu.VMEM((seq_devices // GROUP, HD, GROUP * tok_share), BF16),
            pltpu.VMEM((length, LANES), BF16),
            pltpu.VMEM((seq_devices * CAP, LANES), BF16),
            pltpu.VMEM((HD, length), F32),
            pltpu.VMEM((HD, seq_devices * CAP), F32),
        ],
        compiler_params=params,
        name="attend",
    )(exchange(send))
    hist_out, cand_out = pl.pallas_call(
        functools.partial(output_kernel, tok_share),
        in_specs=[vmem] * 8,
        out_specs=[vmem] * 2,
        out_shape=[
            jax.ShapeDtypeStruct((hist_rows, width), BF16),
            jax.ShapeDtypeStruct((cand_count, width), BF16),
        ],
        scratch_shapes=[pltpu.VMEM((hist_rows + cand_count, width), F32)],
        compiler_params=params,
        name="combine",
    )(exchange(back), assignment, hist, cand, gate, cgate, gain_attn, weight_out)
    return hist_out.reshape(history.shape), cand_out.reshape(candidates.shape)


def solution(mesh):
    in_specs = (
        P(("groups", "dp"), "seq", None),
        P(("groups", "dp"), "seq", None),
        P(("groups", "dp")),
        P(("groups", "dp"), "seq"),
        P(),
        P(),
        P(),
        P(),
    )
    out_specs = (P(("groups", "dp"), "seq", None), P(("groups", "dp"), "seq", None))
    return jax.shard_map(
        per_device, mesh=mesh, in_specs=in_specs, out_specs=out_specs, check_vma=False
    )
```

```python
import functools

import jax
import jax.numpy as jnp
from jax import lax
from jax.experimental import pallas as pl
from jax.experimental.pallas import tpu as pltpu
from jax.sharding import PartitionSpec as P

H = 16
HD = 64
CAP = 40
LANES = 128
CAND_HALF = CAP // 2
CAND_PAD = 24
HEADS_STEP = 16
PARTS = 4
VMEM_LIMIT = 28 << 20
STAGGER_NS = 35_000
GROUP = 8
F32 = jnp.float32
BF16 = jnp.bfloat16


def rms_apply(values, gain):
    return values * lax.rsqrt(jnp.mean(values * values, axis=-1, keepdims=True) + 1e-06) * gain


def silu(values):
    half = values * 0.5
    return half + half * jnp.tanh(half)


def swap_halves(values):
    return pltpu.roll(values, HD, 1)


def low_lanes(rows):
    return lax.broadcasted_iota(jnp.int32, (rows, LANES), 1) < HD


def join(first, second):
    return jnp.where(low_lanes(first.shape[0]), first, second)


def selection(owner_row, member):
    count = owner_row.shape[1]
    mine = (owner_row == member).astype(F32)
    before = (
        lax.broadcasted_iota(jnp.int32, (count, count), 0)
        < lax.broadcasted_iota(jnp.int32, (count, count), 1)
    ).astype(F32)
    rank = jnp.dot(jnp.broadcast_to(mine, (8, count)), before, preferred_element_type=F32)[0:1]
    row = jnp.where(rank < CAND_HALF, rank, rank + (CAND_PAD - CAND_HALF))
    row = jnp.where(mine > 0.5, row, -1.0)
    rows = lax.broadcasted_iota(jnp.int32, (2 * CAND_PAD, count), 0).astype(F32)
    return (rows == row).astype(BF16)


def project_kernel(
    axis,
    stagger_axis,
    tok_share,
    lengths_hbm,
    hist_hbm,
    cand_hbm,
    owner_hbm,
    gain_hbm,
    weight_hbm,
    send_ref,
    gate_ref,
    cgate_ref,
    lengths_ref,
    hist_ref,
    cand_ref,
    owner_ref,
    gain_ref,
    weight_ref,
    normed_ref,
    loaded,
    arrived,
):
    hist_rows, width = hist_ref.shape
    hist_local = hist_rows // tok_share
    half = tok_share // 2
    chunk = tok_share + half + CAND_HALF
    step_width = HEADS_STEP * HD
    steps = H // HEADS_STEP

    def fetch(step, part):
        start = part * width + step * step_width
        return pltpu.make_async_copy(
            weight_hbm.at[:, start : start + step_width],
            weight_ref.at[step, part],
            arrived.at[step, part],
        )

    loads = [
        pltpu.make_async_copy(source, target, loaded.at[number])
        for number, (source, target) in enumerate(
            (
                (gain_hbm, gain_ref),
                (hist_hbm, hist_ref),
                (cand_hbm, cand_ref),
                (owner_hbm, owner_ref),
                (lengths_hbm, lengths_ref),
            )
        )
    ]
    for load in loads:
        load.start()
    for step in range(steps):
        for part in (2, 3, 1, 0):
            fetch(step, part).start()
    for load in loads:
        load.wait()
    @pl.when(lax.axis_index(stagger_axis) > 0)
    def _():
        pl.delay(STAGGER_NS)

    gain = gain_ref[...]
    normed_ref[:hist_rows] = rms_apply(hist_ref[...].astype(F32), gain).astype(BF16)
    normed_ref[hist_rows:] = rms_apply(cand_ref[...].astype(F32), gain).astype(BF16)
    picks = [selection(owner_ref[...], member) for member in range(hist_local)]
    position = lax.axis_index(axis) * tok_share + lax.broadcasted_iota(jnp.int32, (tok_share, LANES), 0)

    for step in range(steps):

        def times(rows, part):
            fetch(step, part).wait()
            return jnp.dot(normed_ref[:rows], weight_ref[step, part], preferred_element_type=F32)

        all_rows = normed_ref.shape[0]
        keys = times(hist_rows, 2)
        values = times(hist_rows, 3)
        query = times(all_rows, 1).astype(BF16).astype(F32) * (0.5 * HD ** (-0.5))
        cand_query = query[hist_rows:].astype(BF16)
        for member in range(hist_local):
            rows = slice(member * tok_share, (member + 1) * tok_share)
            picked = jnp.dot(picks[member], cand_query, preferred_element_type=F32)
            present = position < lengths_ref[member]
            for pair in range(HEADS_STEP // 2):
                lanes = slice(pair * LANES, (pair + 1) * LANES)
                key_slab = jnp.where(present, keys[rows, lanes], 0.0)
                value_slab, query_slab, cand_slab = values[rows, lanes], query[rows, lanes], picked[:, lanes]
                even = (member * H + step * HEADS_STEP + 2 * pair) * chunk
                odd = even + chunk
                send_ref[even : even + tok_share] = join(key_slab, swap_halves(value_slab)).astype(BF16)
                send_ref[odd : odd + tok_share] = join(swap_halves(key_slab), value_slab).astype(BF16)
                top, low = query_slab[:half], query_slab[half:]
                even, odd = even + tok_share, odd + tok_share
                send_ref[even : even + half] = join(top, swap_halves(low)).astype(BF16)
                send_ref[odd : odd + half] = join(swap_halves(top), low).astype(BF16)
                top, low = cand_slab[:CAND_PAD], cand_slab[CAND_PAD:]
                even, odd = even + half, odd + half
                send_ref[even : even + CAND_HALF] = join(top, swap_halves(low)).astype(BF16)[:CAND_HALF]
                send_ref[odd : odd + CAND_HALF] = join(swap_halves(top), low).astype(BF16)[:CAND_HALF]
        gate = silu(times(all_rows, 0)).astype(BF16)
        columns = slice(step * step_width, (step + 1) * step_width)
        gate_ref[:, columns] = gate[:hist_rows]
        cgate_ref[:, columns] = gate[hist_rows:]


def attend_kernel(tok_share, recv_ref, back_ref, kv_ref, vt_ref, q_ref, cq_ref, ot_ref, ct_ref):
    half = tok_share // 2
    chunk, back_chunk = tok_share + half + CAND_HALF, half + CAND_HALF
    sources = recv_ref.shape[0] // chunk
    groups = sources // GROUP
    keys_group, half_group = GROUP * tok_share, GROUP * half
    queries_group = 2 * half_group
    cands = sources * CAND_HALF

    def keys_of(group):
        return kv_ref[group * keys_group : (group + 1) * keys_group]

    def low_half(values):
        return jnp.where(low_lanes(values.shape[0]), values, 0.0).astype(BF16)

    for source in range(sources):
        base = source * chunk
        kv_ref[source * tok_share : (source + 1) * tok_share] = recv_ref[base : base + tok_share]
        base = base + tok_share
        packed = recv_ref[base : base + half].astype(F32)
        place = source // GROUP * queries_group + source % GROUP * half
        q_ref[place : place + half] = low_half(packed)
        q_ref[place + half_group : place + half_group + half] = low_half(swap_halves(packed))
        base = base + half
        packed = recv_ref[base : base + CAND_HALF].astype(F32)
        place = source * CAND_HALF
        cq_ref[place : place + CAND_HALF] = low_half(packed)
        cq_ref[cands + place : cands + place + CAND_HALF] = low_half(swap_halves(packed))
    for group in range(groups):
        vt_ref[group] = keys_of(group).T[HD:]

    def weigh(group, query, allowed=None):
        half_score = lax.dot_general(
            keys_of(group), query, (((1,), (1,)), ((), ())), preferred_element_type=F32
        )
        weight = half_score + half_score * jnp.tanh(half_score)
        if allowed is not None:
            weight = jnp.where(allowed, weight, 0.0)
        return jnp.dot(vt_ref[group], weight.astype(BF16), preferred_element_type=F32)

    for group in range(groups):
        part = weigh(group, cq_ref[...])
        ct_ref[...] = part if group == 0 else ct_ref[...] + part

    column = lax.broadcasted_iota(jnp.int32, (1, queries_group), 1)
    is_low = (column >= half_group).astype(jnp.int32)
    column = column - is_low * half_group
    source = jnp.zeros_like(column)
    for later in range(1, GROUP):
        source = source + (column >= later * half).astype(jnp.int32)
    position = source * half + column + is_low * half
    causal = lax.broadcasted_iota(jnp.int32, (keys_group, queries_group), 0) <= position
    for group in range(groups):
        base = group * queries_group
        own = slice(base, base + queries_group)
        part = weigh(group, q_ref[own], causal)
        ot_ref[:, own] = part if group == 0 else ot_ref[:, own] + part
        if group + 1 < groups:
            later = slice(base + queries_group, groups * queries_group)
            part = weigh(group, q_ref[later])
            ot_ref[:, later] = part if group == 0 else ot_ref[:, later] + part

    for group in range(groups):
        base = group * queries_group
        top = ot_ref[:, base : base + half_group]
        low = ot_ref[:, base + half_group : base + queries_group]
        joined = jnp.concatenate([top, low], axis=0).T.astype(BF16)
        for member in range(GROUP):
            place = (group * GROUP + member) * back_chunk
            back_ref[place : place + half] = joined[member * half : (member + 1) * half]
    joined = jnp.concatenate([ct_ref[:, :cands], ct_ref[:, cands:]], axis=0).T.astype(BF16)
    for source in range(sources):
        place = source * back_chunk + half
        back_ref[place : place + CAND_HALF] = joined[source * CAND_HALF : (source + 1) * CAND_HALF]


def output_kernel(
    tok_share,
    back_ref,
    owner_ref,
    hist_ref,
    cand_ref,
    gate_ref,
    cgate_ref,
    gain_ref,
    weight_ref,
    hist_out_ref,
    cand_out_ref,
    rows_ref,
):
    half = tok_share // 2
    hist_rows = hist_ref.shape[0]
    hist_local = hist_rows // tok_share
    cand_rows = cand_ref.shape[0]
    chunk = half + CAND_HALF
    picks = [selection(owner_ref[...], member) for member in range(hist_local)]
    fill = jnp.zeros((CAND_PAD - CAND_HALF, LANES), F32)
    for pair in range(H // 2):
        lanes = slice(pair * LANES, (pair + 1) * LANES)
        cross_slab = jnp.zeros((cand_rows, LANES), F32)
        for member in range(hist_local):
            base = member * tok_share
            first = (member * H + 2 * pair) * chunk
            even = back_ref[first : first + half].astype(F32)
            odd = back_ref[first + chunk : first + chunk + half].astype(F32)
            rows_ref[base : base + half, lanes] = join(even, swap_halves(odd))
            rows_ref[base + half : base + tok_share, lanes] = join(swap_halves(even), odd)
            first = first + half
            even = back_ref[first : first + CAND_HALF].astype(F32)
            odd = back_ref[first + chunk : first + chunk + CAND_HALF].astype(F32)
            upper, lower = join(even, swap_halves(odd)), join(swap_halves(even), odd)
            found = jnp.concatenate([upper, fill, lower, fill], axis=0).astype(BF16)
            cross_slab = cross_slab + lax.dot_general(
                picks[member], found, (((0,), (0,)), ((), ())), preferred_element_type=F32
            )
        rows_ref[hist_rows:, lanes] = cross_slab
    gain = gain_ref[...]
    attended = rows_ref[...]
    scaled = rms_apply(attended, gain)
    hist_gated = (scaled[:hist_rows] * gate_ref[...].astype(F32)).astype(BF16)
    cand_gated = (scaled[hist_rows:] * cgate_ref[...].astype(F32)).astype(BF16)
    gated = jnp.concatenate([hist_gated, cand_gated], axis=0)
    product = jnp.dot(gated, weight_ref[...], preferred_element_type=F32)
    hist_out_ref[...] = (hist_ref[...].astype(F32) + product[:hist_rows]).astype(BF16)
    cand_out_ref[...] = (cand_ref[...].astype(F32) + product[hist_rows:]).astype(BF16)


def per_device(history, candidates, lengths, assignment, weight_in, weight_out, gain_in, gain_attn):
    seq_devices = lax.axis_size("seq")
    hist_local, tok_share, width = history.shape
    cand_count = candidates.shape[1]
    half = tok_share // 2
    hist_rows = hist_local * tok_share
    items = hist_local * H
    assert items == seq_devices
    hist = history.reshape(hist_rows, width)
    cand = candidates.reshape(cand_count, width)
    gain_in = gain_in.reshape(1, width)
    gain_attn = gain_attn.reshape(1, width)
    send_rows, back_rows = tok_share + half + CAND_HALF, half + CAND_HALF
    length = seq_devices * tok_share
    params = pltpu.CompilerParams(vmem_limit_bytes=VMEM_LIMIT)
    vmem = pl.BlockSpec(memory_space=pltpu.VMEM)

    def exchange(rows):
        pairs = rows.reshape(items, rows.shape[0] // items // 2, 2, LANES)
        moved = lax.all_to_all(pairs, "seq", split_axis=0, concat_axis=0, tiled=True)
        return pltpu.with_memory_space_constraint(moved.reshape(rows.shape), pltpu.VMEM)

    send, gate, cgate = pl.pallas_call(
        functools.partial(project_kernel, "seq", "dp", tok_share),
        in_specs=[pl.BlockSpec(memory_space=pltpu.HBM)] * 6,
        out_specs=[vmem] * 3,
        out_shape=[
            pltpu.VMEM((items * send_rows, LANES), BF16),
            jax.ShapeDtypeStruct((hist_rows, width), BF16),
            jax.ShapeDtypeStruct((cand_count, width), BF16),
        ],
        scratch_shapes=[
            pltpu.SMEM(lengths.shape, lengths.dtype),
            pltpu.VMEM(hist.shape, BF16),
            pltpu.VMEM(cand.shape, BF16),
            pltpu.VMEM(assignment.shape, assignment.dtype),
            pltpu.VMEM(gain_in.shape, F32),
            pltpu.VMEM((H // HEADS_STEP, PARTS, width, HEADS_STEP * HD), BF16),
            pltpu.VMEM((hist_rows + cand_count, width), BF16),
            pltpu.SemaphoreType.DMA((5,)),
            pltpu.SemaphoreType.DMA((H // HEADS_STEP, PARTS)),
        ],
        compiler_params=params,
        name="project",
    )(
        *(
            pltpu.with_memory_space_constraint(argument, pltpu.HBM)
            for argument in (lengths, hist, cand, assignment, gain_in, weight_in)
        )
    )
    back = pl.pallas_call(
        functools.partial(attend_kernel, tok_share),
        in_specs=[vmem],
        out_specs=vmem,
        out_shape=pltpu.VMEM((items * back_rows, LANES), BF16),
        scratch_shapes=[
            pltpu.VMEM((length, LANES), BF16),
            pltpu.VMEM((seq_devices // GROUP, HD, GROUP * tok_share), BF16),
            pltpu.VMEM((length, LANES), BF16),
            pltpu.VMEM((seq_devices * CAP, LANES), BF16),
            pltpu.VMEM((HD, length), F32),
            pltpu.VMEM((HD, seq_devices * CAP), F32),
        ],
        compiler_params=params,
        name="attend",
    )(exchange(send))
    hist_out, cand_out = pl.pallas_call(
        functools.partial(output_kernel, tok_share),
        in_specs=[vmem] * 8,
        out_specs=[vmem] * 2,
        out_shape=[
            jax.ShapeDtypeStruct((hist_rows, width), BF16),
            jax.ShapeDtypeStruct((cand_count, width), BF16),
        ],
        scratch_shapes=[pltpu.VMEM((hist_rows + cand_count, width), F32)],
        compiler_params=params,
        name="combine",
    )(exchange(back), assignment, hist, cand, gate, cgate, gain_attn, weight_out)
    return hist_out.reshape(history.shape), cand_out.reshape(candidates.shape)


def solution(mesh):
    in_specs = (
        P(("groups", "dp"), "seq", None),
        P(("groups", "dp"), "seq", None),
        P(("groups", "dp")),
        P(("groups", "dp"), "seq"),
        P(),
        P(),
        P(),
        P(),
    )
    out_specs = (P(("groups", "dp"), "seq", None), P(("groups", "dp"), "seq", None))
    return jax.shard_map(
        per_device, mesh=mesh, in_specs=in_specs, out_specs=out_specs, check_vma=False
    )
```

```python
import functools

import jax
import jax.numpy as jnp
from jax import lax
from jax.experimental import pallas as pl
from jax.experimental.pallas import tpu as pltpu
from jax.sharding import PartitionSpec as P

H = 16
HD = 64
CAP = 40
LANES = 128
CAND_HALF = CAP // 2
CAND_PAD = 24
HEADS_STEP = 16
PARTS = 4
VMEM_LIMIT = 28 << 20
STAGGER_NS = 35_000
GROUP = 8
F32 = jnp.float32
BF16 = jnp.bfloat16


def rms_apply(values, gain):
    return values * lax.rsqrt(jnp.mean(values * values, axis=-1, keepdims=True) + 1e-06) * gain


def silu(values):
    half = values * 0.5
    return half + half * jnp.tanh(half)


def swap_halves(values):
    return pltpu.roll(values, HD, 1)


def low_lanes(rows):
    return lax.broadcasted_iota(jnp.int32, (rows, LANES), 1) < HD


def join(first, second):
    return jnp.where(low_lanes(first.shape[0]), first, second)


def selection(owner_row, member):
    count = owner_row.shape[1]
    mine = (owner_row == member).astype(F32)
    before = (
        lax.broadcasted_iota(jnp.int32, (count, count), 0)
        < lax.broadcasted_iota(jnp.int32, (count, count), 1)
    ).astype(F32)
    rank = jnp.dot(jnp.broadcast_to(mine, (8, count)), before, preferred_element_type=F32)[0:1]
    row = jnp.where(rank < CAND_HALF, rank, rank + (CAND_PAD - CAND_HALF))
    row = jnp.where(mine > 0.5, row, -1.0)
    rows = lax.broadcasted_iota(jnp.int32, (2 * CAND_PAD, count), 0).astype(F32)
    return (rows == row).astype(BF16)


def project_kernel(
    axis,
    stagger_axis,
    tok_share,
    lengths_hbm,
    hist_hbm,
    cand_hbm,
    owner_hbm,
    gain_hbm,
    weight_hbm,
    send_ref,
    normed_ref,
    gate_ref,
    lengths_ref,
    hist_ref,
    cand_ref,
    owner_ref,
    gain_ref,
    weight_ref,
    loaded,
    arrived,
):
    hist_rows, width = hist_ref.shape
    hist_local = hist_rows // tok_share
    half = tok_share // 2
    chunk = tok_share + half + CAND_HALF
    step_width = HEADS_STEP * HD
    steps = H // HEADS_STEP

    def fetch(step, part):
        start = part * width + step * step_width
        return pltpu.make_async_copy(
            weight_hbm.at[:, start : start + step_width],
            weight_ref.at[step, part],
            arrived.at[step, part],
        )

    loads = [
        pltpu.make_async_copy(source, target, loaded.at[number])
        for number, (source, target) in enumerate(
            (
                (gain_hbm, gain_ref),
                (hist_hbm, hist_ref),
                (cand_hbm, cand_ref),
                (owner_hbm, owner_ref),
                (lengths_hbm, lengths_ref),
            )
        )
    ]
    for load in loads:
        load.start()
    for step in range(steps):
        for part in (2, 3, 1):
            fetch(step, part).start()
    for load in loads:
        load.wait()
    gain = gain_ref[...]
    normed_ref[:hist_rows] = rms_apply(hist_ref[...].astype(F32), gain).astype(BF16)
    normed_ref[hist_rows:] = rms_apply(cand_ref[...].astype(F32), gain).astype(BF16)
    picks = [selection(owner_ref[...], member) for member in range(hist_local)]
    position = lax.axis_index(axis) * tok_share + lax.broadcasted_iota(jnp.int32, (tok_share, LANES), 0)

    def times(step, rows, part):
        fetch(step, part).wait()
        return jnp.dot(normed_ref[:rows], weight_ref[step, part], preferred_element_type=F32)

    for step in range(steps):
        keys = times(step, hist_rows, 2)
        values = times(step, hist_rows, 3)
        query = times(step, normed_ref.shape[0], 1).astype(BF16).astype(F32) * (0.5 * HD ** (-0.5))
        cand_query = query[hist_rows:].astype(BF16)
        for member in range(hist_local):
            rows = slice(member * tok_share, (member + 1) * tok_share)
            picked = jnp.dot(picks[member], cand_query, preferred_element_type=F32)
            present = position < lengths_ref[member]
            for pair in range(HEADS_STEP // 2):
                lanes = slice(pair * LANES, (pair + 1) * LANES)
                key_slab = jnp.where(present, keys[rows, lanes], 0.0)
                value_slab, query_slab, cand_slab = values[rows, lanes], query[rows, lanes], picked[:, lanes]
                even = (member * H + step * HEADS_STEP + 2 * pair) * chunk
                odd = even + chunk
                send_ref[even : even + tok_share] = join(key_slab, swap_halves(value_slab)).astype(BF16)
                send_ref[odd : odd + tok_share] = join(swap_halves(key_slab), value_slab).astype(BF16)
                top, low = query_slab[:half], query_slab[half:]
                even, odd = even + tok_share, odd + tok_share
                send_ref[even : even + half] = join(top, swap_halves(low)).astype(BF16)
                send_ref[odd : odd + half] = join(swap_halves(top), low).astype(BF16)
                top, low = cand_slab[:CAND_PAD], cand_slab[CAND_PAD:]
                even, odd = even + half, odd + half
                send_ref[even : even + CAND_HALF] = join(top, swap_halves(low)).astype(BF16)[:CAND_HALF]
                send_ref[odd : odd + CAND_HALF] = join(swap_halves(top), low).astype(BF16)[:CAND_HALF]

    @pl.when(lax.axis_index(stagger_axis) > 0)
    def _():
        for step in range(steps):
            fetch(step, 0).start()
        for step in range(steps):
            columns = slice(step * step_width, (step + 1) * step_width)
            gate_ref[:, columns] = silu(times(step, normed_ref.shape[0], 0)).astype(BF16)
        pl.delay(STAGGER_NS)


def attend_kernel(tok_share, recv_ref, back_ref, kv_ref, vt_ref, q_ref, cq_ref, ot_ref, ct_ref):
    half = tok_share // 2
    chunk, back_chunk = tok_share + half + CAND_HALF, half + CAND_HALF
    sources = recv_ref.shape[0] // chunk
    groups = sources // GROUP
    keys_group, half_group = GROUP * tok_share, GROUP * half
    queries_group = 2 * half_group
    cands = sources * CAND_HALF

    def keys_of(group):
        return kv_ref[group * keys_group : (group + 1) * keys_group]

    def low_half(values):
        return jnp.where(low_lanes(values.shape[0]), values, 0.0).astype(BF16)

    for source in range(sources):
        base = source * chunk
        kv_ref[source * tok_share : (source + 1) * tok_share] = recv_ref[base : base + tok_share]
        base = base + tok_share
        packed = recv_ref[base : base + half].astype(F32)
        place = source // GROUP * queries_group + source % GROUP * half
        q_ref[place : place + half] = low_half(packed)
        q_ref[place + half_group : place + half_group + half] = low_half(swap_halves(packed))
        base = base + half
        packed = recv_ref[base : base + CAND_HALF].astype(F32)
        place = source * CAND_HALF
        cq_ref[place : place + CAND_HALF] = low_half(packed)
        cq_ref[cands + place : cands + place + CAND_HALF] = low_half(swap_halves(packed))
    for group in range(groups):
        vt_ref[group] = keys_of(group).T[HD:]

    def weigh(group, query, allowed=None):
        half_score = lax.dot_general(
            keys_of(group), query, (((1,), (1,)), ((), ())), preferred_element_type=F32
        )
        weight = half_score + half_score * jnp.tanh(half_score)
        if allowed is not None:
            weight = jnp.where(allowed, weight, 0.0)
        return jnp.dot(vt_ref[group], weight.astype(BF16), preferred_element_type=F32)

    for group in range(groups):
        part = weigh(group, cq_ref[...])
        ct_ref[...] = part if group == 0 else ct_ref[...] + part

    column = lax.broadcasted_iota(jnp.int32, (1, queries_group), 1)
    is_low = (column >= half_group).astype(jnp.int32)
    column = column - is_low * half_group
    source = jnp.zeros_like(column)
    for later in range(1, GROUP):
        source = source + (column >= later * half).astype(jnp.int32)
    position = source * half + column + is_low * half
    causal = lax.broadcasted_iota(jnp.int32, (keys_group, queries_group), 0) <= position
    for group in range(groups):
        base = group * queries_group
        own = slice(base, base + queries_group)
        part = weigh(group, q_ref[own], causal)
        ot_ref[:, own] = part if group == 0 else ot_ref[:, own] + part
        for after in range(group + 1, groups):
            later = slice(after * queries_group, (after + 1) * queries_group)
            part = weigh(group, q_ref[later])
            ot_ref[:, later] = part if group == 0 else ot_ref[:, later] + part

    for group in range(groups):
        base = group * queries_group
        top = ot_ref[:, base : base + half_group]
        low = ot_ref[:, base + half_group : base + queries_group]
        joined = jnp.concatenate([top, low], axis=0).T.astype(BF16)
        for member in range(GROUP):
            place = (group * GROUP + member) * back_chunk
            back_ref[place : place + half] = joined[member * half : (member + 1) * half]
    joined = jnp.concatenate([ct_ref[:, :cands], ct_ref[:, cands:]], axis=0).T.astype(BF16)
    for source in range(sources):
        place = source * back_chunk + half
        back_ref[place : place + CAND_HALF] = joined[source * CAND_HALF : (source + 1) * CAND_HALF]


def output_kernel(
    stagger_axis,
    tok_share,
    back_ref,
    owner_ref,
    hist_ref,
    cand_ref,
    normed_ref,
    given_ref,
    gain_ref,
    weight_ref,
    weight_in_hbm,
    hist_out_ref,
    cand_out_ref,
    rows_ref,
    gate_ref,
    gate_weight_ref,
    arrived,
):
    width = hist_ref.shape[1]
    is_first = lax.axis_index(stagger_axis) == 0

    @pl.when(is_first)
    def _():
        fetch = pltpu.make_async_copy(weight_in_hbm.at[:, :width], gate_weight_ref, arrived)
        fetch.start()
        fetch.wait()
        product = jnp.dot(normed_ref[...], gate_weight_ref[...], preferred_element_type=F32)
        gate_ref[...] = silu(product).astype(BF16)

    @pl.when(jnp.logical_not(is_first))
    def _():
        gate_ref[...] = given_ref[...]

    half = tok_share // 2
    hist_rows = hist_ref.shape[0]
    hist_local = hist_rows // tok_share
    cand_rows = cand_ref.shape[0]
    chunk = half + CAND_HALF
    picks = [selection(owner_ref[...], member) for member in range(hist_local)]
    fill = jnp.zeros((CAND_PAD - CAND_HALF, LANES), F32)
    for pair in range(H // 2):
        lanes = slice(pair * LANES, (pair + 1) * LANES)
        cross_slab = jnp.zeros((cand_rows, LANES), F32)
        for member in range(hist_local):
            base = member * tok_share
            first = (member * H + 2 * pair) * chunk
            even = back_ref[first : first + half].astype(F32)
            odd = back_ref[first + chunk : first + chunk + half].astype(F32)
            rows_ref[base : base + half, lanes] = join(even, swap_halves(odd))
            rows_ref[base + half : base + tok_share, lanes] = join(swap_halves(even), odd)
            first = first + half
            even = back_ref[first : first + CAND_HALF].astype(F32)
            odd = back_ref[first + chunk : first + chunk + CAND_HALF].astype(F32)
            upper, lower = join(even, swap_halves(odd)), join(swap_halves(even), odd)
            found = jnp.concatenate([upper, fill, lower, fill], axis=0).astype(BF16)
            cross_slab = cross_slab + lax.dot_general(
                picks[member], found, (((0,), (0,)), ((), ())), preferred_element_type=F32
            )
        rows_ref[hist_rows:, lanes] = cross_slab
    gain = gain_ref[...]
    attended = rows_ref[...]
    scaled = rms_apply(attended, gain)
    gated = (scaled * gate_ref[...].astype(F32)).astype(BF16)
    product = jnp.dot(gated, weight_ref[...], preferred_element_type=F32)
    hist_out_ref[...] = (hist_ref[...].astype(F32) + product[:hist_rows]).astype(BF16)
    cand_out_ref[...] = (cand_ref[...].astype(F32) + product[hist_rows:]).astype(BF16)


def per_device(history, candidates, lengths, assignment, weight_in, weight_out, gain_in, gain_attn):
    seq_devices = lax.axis_size("seq")
    hist_local, tok_share, width = history.shape
    cand_count = candidates.shape[1]
    half = tok_share // 2
    hist_rows = hist_local * tok_share
    items = hist_local * H
    assert items == seq_devices
    hist = history.reshape(hist_rows, width)
    cand = candidates.reshape(cand_count, width)
    gain_in = gain_in.reshape(1, width)
    gain_attn = gain_attn.reshape(1, width)
    send_rows, back_rows = tok_share + half + CAND_HALF, half + CAND_HALF
    length = seq_devices * tok_share
    params = pltpu.CompilerParams(vmem_limit_bytes=VMEM_LIMIT)
    vmem = pl.BlockSpec(memory_space=pltpu.VMEM)

    def exchange(rows):
        pairs = rows.reshape(items, rows.shape[0] // items // 2, 2, LANES)
        moved = lax.all_to_all(pairs, "seq", split_axis=0, concat_axis=0, tiled=True)
        return pltpu.with_memory_space_constraint(moved.reshape(rows.shape), pltpu.VMEM)

    all_rows = hist_rows + cand_count
    send, normed, gate = pl.pallas_call(
        functools.partial(project_kernel, "seq", "dp", tok_share),
        in_specs=[pl.BlockSpec(memory_space=pltpu.HBM)] * 6,
        out_specs=[vmem] * 3,
        out_shape=[
            pltpu.VMEM((items * send_rows, LANES), BF16),
            pltpu.VMEM((all_rows, width), BF16),
            jax.ShapeDtypeStruct((all_rows, width), BF16),
        ],
        scratch_shapes=[
            pltpu.SMEM(lengths.shape, lengths.dtype),
            pltpu.VMEM(hist.shape, BF16),
            pltpu.VMEM(cand.shape, BF16),
            pltpu.VMEM(assignment.shape, assignment.dtype),
            pltpu.VMEM(gain_in.shape, F32),
            pltpu.VMEM((H // HEADS_STEP, PARTS, width, HEADS_STEP * HD), BF16),
            pltpu.SemaphoreType.DMA((5,)),
            pltpu.SemaphoreType.DMA((H // HEADS_STEP, PARTS)),
        ],
        compiler_params=params,
        name="project",
    )(
        *(
            pltpu.with_memory_space_constraint(argument, pltpu.HBM)
            for argument in (lengths, hist, cand, assignment, gain_in, weight_in)
        )
    )
    back = pl.pallas_call(
        functools.partial(attend_kernel, tok_share),
        in_specs=[vmem],
        out_specs=vmem,
        out_shape=pltpu.VMEM((items * back_rows, LANES), BF16),
        scratch_shapes=[
            pltpu.VMEM((length, LANES), BF16),
            pltpu.VMEM((seq_devices // GROUP, HD, GROUP * tok_share), BF16),
            pltpu.VMEM((length, LANES), BF16),
            pltpu.VMEM((seq_devices * CAP, LANES), BF16),
            pltpu.VMEM((HD, length), F32),
            pltpu.VMEM((HD, seq_devices * CAP), F32),
        ],
        compiler_params=params,
        name="attend",
    )(exchange(send))
    hist_out, cand_out = pl.pallas_call(
        functools.partial(output_kernel, "dp", tok_share),
        in_specs=[vmem] * 8 + [pl.BlockSpec(memory_space=pltpu.HBM)],
        out_specs=[vmem] * 2,
        out_shape=[
            jax.ShapeDtypeStruct((hist_rows, width), BF16),
            jax.ShapeDtypeStruct((cand_count, width), BF16),
        ],
        scratch_shapes=[
            pltpu.VMEM((all_rows, width), F32),
            pltpu.VMEM((all_rows, width), BF16),
            pltpu.VMEM((width, width), BF16),
            pltpu.SemaphoreType.DMA,
        ],
        compiler_params=params,
        name="combine",
    )(
        exchange(back),
        assignment,
        hist,
        cand,
        normed,
        gate,
        gain_attn,
        weight_out,
        pltpu.with_memory_space_constraint(weight_in, pltpu.HBM),
    )
    return hist_out.reshape(history.shape), cand_out.reshape(candidates.shape)


def solution(mesh):
    in_specs = (
        P(("groups", "dp"), "seq", None),
        P(("groups", "dp"), "seq", None),
        P(("groups", "dp")),
        P(("groups", "dp"), "seq"),
        P(),
        P(),
        P(),
        P(),
    )
    out_specs = (P(("groups", "dp"), "seq", None), P(("groups", "dp"), "seq", None))
    return jax.shard_map(
        per_device, mesh=mesh, in_specs=in_specs, out_specs=out_specs, check_vma=False
    )
```

```python
import functools

import jax
import jax.numpy as jnp
from jax import lax
from jax.experimental import pallas as pl
from jax.experimental.pallas import tpu as pltpu
from jax.sharding import PartitionSpec as P

H = 16
HD = 64
CAP = 40
LANES = 128
CAND_HALF = CAP // 2
CAND_PAD = 24
HEADS_STEP = 16
PARTS = 4
VMEM_LIMIT = 28 << 20
STAGGER_NS = 32_000
WEIGHTS_AHEAD = 2
GROUP = 8
F32 = jnp.float32
BF16 = jnp.bfloat16


def rms_apply(values, gain):
    return values * lax.rsqrt(jnp.mean(values * values, axis=-1, keepdims=True) + 1e-06) * gain


def silu(values):
    half = values * 0.5
    return half + half * jnp.tanh(half)


def swap_halves(values):
    return pltpu.roll(values, HD, 1)


def low_lanes(rows):
    return lax.broadcasted_iota(jnp.int32, (rows, LANES), 1) < HD


def join(first, second):
    return jnp.where(low_lanes(first.shape[0]), first, second)


def selection(owner_row, member):
    count = owner_row.shape[1]
    mine = (owner_row == member).astype(F32)
    before = (
        lax.broadcasted_iota(jnp.int32, (count, count), 0)
        < lax.broadcasted_iota(jnp.int32, (count, count), 1)
    ).astype(F32)
    rank = jnp.dot(jnp.broadcast_to(mine, (8, count)), before, preferred_element_type=F32)[0:1]
    row = jnp.where(rank < CAND_HALF, rank, rank + (CAND_PAD - CAND_HALF))
    row = jnp.where(mine > 0.5, row, -1.0)
    rows = lax.broadcasted_iota(jnp.int32, (2 * CAND_PAD, count), 0).astype(F32)
    return (rows == row).astype(BF16)


def project_kernel(
    axis,
    stagger_axis,
    tok_share,
    lengths_hbm,
    hist_hbm,
    cand_hbm,
    owner_hbm,
    gain_hbm,
    weight_hbm,
    send_ref,
    normed_ref,
    gate_ref,
    lengths_ref,
    hist_ref,
    cand_ref,
    owner_ref,
    gain_ref,
    weight_ref,
    loaded,
    arrived,
):
    hist_rows, width = hist_ref.shape
    hist_local = hist_rows // tok_share
    half = tok_share // 2
    chunk = tok_share + half + CAND_HALF
    step_width = HEADS_STEP * HD
    steps = H // HEADS_STEP

    def fetch(step, part):
        start = part * width + step * step_width
        return pltpu.make_async_copy(
            weight_hbm.at[:, start : start + step_width],
            weight_ref.at[step, part],
            arrived.at[step, part],
        )

    loads = [
        pltpu.make_async_copy(source, target, loaded.at[number])
        for number, (source, target) in enumerate(
            (
                (gain_hbm, gain_ref),
                (hist_hbm, hist_ref),
                (cand_hbm, cand_ref),
                (owner_hbm, owner_ref),
                (lengths_hbm, lengths_ref),
            )
        )
    ]
    for load in loads:
        load.start()
    for step in range(steps):
        for part in (2, 3, 1):
            fetch(step, part).start()
    for load in loads:
        load.wait()
    gain = gain_ref[...]
    normed_ref[:hist_rows] = rms_apply(hist_ref[...].astype(F32), gain).astype(BF16)
    normed_ref[hist_rows:] = rms_apply(cand_ref[...].astype(F32), gain).astype(BF16)
    picks = [selection(owner_ref[...], member) for member in range(hist_local)]
    position = lax.axis_index(axis) * tok_share + lax.broadcasted_iota(jnp.int32, (tok_share, LANES), 0)

    def times(step, rows, part):
        fetch(step, part).wait()
        return jnp.dot(normed_ref[:rows], weight_ref[step, part], preferred_element_type=F32)

    for step in range(steps):
        keys = times(step, hist_rows, 2)
        values = times(step, hist_rows, 3)
        query = times(step, normed_ref.shape[0], 1).astype(BF16).astype(F32) * (0.5 * HD ** (-0.5))
        cand_query = query[hist_rows:].astype(BF16)
        for member in range(hist_local):
            rows = slice(member * tok_share, (member + 1) * tok_share)
            picked = jnp.dot(picks[member], cand_query, preferred_element_type=F32)
            present = position < lengths_ref[member]
            for pair in range(HEADS_STEP // 2):
                lanes = slice(pair * LANES, (pair + 1) * LANES)
                key_slab = jnp.where(present, keys[rows, lanes], 0.0)
                value_slab, query_slab, cand_slab = values[rows, lanes], query[rows, lanes], picked[:, lanes]
                even = (member * H + step * HEADS_STEP + 2 * pair) * chunk
                odd = even + chunk
                send_ref[even : even + tok_share] = join(key_slab, swap_halves(value_slab)).astype(BF16)
                send_ref[odd : odd + tok_share] = join(swap_halves(key_slab), value_slab).astype(BF16)
                top, low = query_slab[:half], query_slab[half:]
                even, odd = even + tok_share, odd + tok_share
                send_ref[even : even + half] = join(top, swap_halves(low)).astype(BF16)
                send_ref[odd : odd + half] = join(swap_halves(top), low).astype(BF16)
                top, low = cand_slab[:CAND_PAD], cand_slab[CAND_PAD:]
                even, odd = even + half, odd + half
                send_ref[even : even + CAND_HALF] = join(top, swap_halves(low)).astype(BF16)[:CAND_HALF]
                send_ref[odd : odd + CAND_HALF] = join(swap_halves(top), low).astype(BF16)[:CAND_HALF]

    @pl.when(lax.axis_index(stagger_axis) > 0)
    def _():
        for step in range(steps):
            fetch(step, 0).start()
        for step in range(steps):
            columns = slice(step * step_width, (step + 1) * step_width)
            gate_ref[:, columns] = silu(times(step, normed_ref.shape[0], 0)).astype(BF16)
        pl.delay(STAGGER_NS)


def attend_kernel(tok_share, recv_ref, back_ref, kv_ref, vt_ref, q_ref, cq_ref, ot_ref, ct_ref):
    half = tok_share // 2
    chunk, back_chunk = tok_share + half + CAND_HALF, half + CAND_HALF
    sources = recv_ref.shape[0] // chunk
    groups = sources // GROUP
    keys_group, half_group = GROUP * tok_share, GROUP * half
    queries_group = 2 * half_group
    cands = sources * CAND_HALF

    def keys_of(group):
        return kv_ref[group * keys_group : (group + 1) * keys_group]

    def low_half(values):
        return jnp.where(low_lanes(values.shape[0]), values, 0.0).astype(BF16)

    for source in range(sources):
        base = source * chunk
        kv_ref[source * tok_share : (source + 1) * tok_share] = recv_ref[base : base + tok_share]
        base = base + tok_share
        packed = recv_ref[base : base + half].astype(F32)
        place = source // GROUP * queries_group + source % GROUP * half
        q_ref[place : place + half] = low_half(packed)
        q_ref[place + half_group : place + half_group + half] = low_half(swap_halves(packed))
        base = base + half
        packed = recv_ref[base : base + CAND_HALF].astype(F32)
        place = source * CAND_HALF
        cq_ref[place : place + CAND_HALF] = low_half(packed)
        cq_ref[cands + place : cands + place + CAND_HALF] = low_half(swap_halves(packed))
    for group in range(groups):
        vt_ref[group] = keys_of(group).T[HD:]

    column = lax.broadcasted_iota(jnp.int32, (1, queries_group), 1)
    is_low = (column >= half_group).astype(jnp.int32)
    column = column - is_low * half_group
    source = jnp.zeros_like(column)
    for later in range(1, GROUP):
        source = source + (column >= later * half).astype(jnp.int32)
    position = source * half + column + is_low * half
    causal = lax.broadcasted_iota(jnp.int32, (keys_group, queries_group), 0) <= position

    def weights(group, query, allowed):
        half_score = lax.dot_general(
            keys_of(group), query, (((1,), (1,)), ((), ())), preferred_element_type=F32
        )
        weight = half_score + half_score * jnp.tanh(half_score)
        if allowed is not None:
            weight = jnp.where(allowed, weight, 0.0)
        return weight.astype(BF16)

    def gather(ref, columns, group, weight, first):
        part = jnp.dot(vt_ref[group], weight, preferred_element_type=F32)
        ref[:, columns] = part if first else ref[:, columns] + part

    work = [(ct_ref, slice(0, 2 * cands), group, cq_ref, None, group == 0) for group in range(groups)]
    for group in range(groups):
        for after in range(group, groups):
            columns = slice(after * queries_group, (after + 1) * queries_group)
            work.append((ot_ref, columns, group, q_ref, causal if after == group else None, group == 0))
    pending = []
    for ref, columns, group, query_ref, allowed, first in work:
        pending.append((ref, columns, group, weights(group, query_ref[columns], allowed), first))
        if len(pending) > WEIGHTS_AHEAD:
            gather(*pending.pop(0))
    for waiting in pending:
        gather(*waiting)

    for group in range(groups):
        base = group * queries_group
        top = ot_ref[:, base : base + half_group]
        low = ot_ref[:, base + half_group : base + queries_group]
        joined = jnp.concatenate([top, low], axis=0).T.astype(BF16)
        for member in range(GROUP):
            place = (group * GROUP + member) * back_chunk
            back_ref[place : place + half] = joined[member * half : (member + 1) * half]
    joined = jnp.concatenate([ct_ref[:, :cands], ct_ref[:, cands:]], axis=0).T.astype(BF16)
    for source in range(sources):
        place = source * back_chunk + half
        back_ref[place : place + CAND_HALF] = joined[source * CAND_HALF : (source + 1) * CAND_HALF]


def output_kernel(
    stagger_axis,
    tok_share,
    back_ref,
    owner_ref,
    hist_ref,
    cand_ref,
    normed_ref,
    given_ref,
    gain_ref,
    weight_ref,
    weight_in_hbm,
    hist_out_ref,
    cand_out_ref,
    rows_ref,
    gate_ref,
    gate_weight_ref,
    arrived,
):
    width = hist_ref.shape[1]
    is_first = lax.axis_index(stagger_axis) == 0

    @pl.when(is_first)
    def _():
        fetch = pltpu.make_async_copy(weight_in_hbm.at[:, :width], gate_weight_ref, arrived)
        fetch.start()
        fetch.wait()
        product = jnp.dot(normed_ref[...], gate_weight_ref[...], preferred_element_type=F32)
        gate_ref[...] = silu(product).astype(BF16)

    @pl.when(jnp.logical_not(is_first))
    def _():
        gate_ref[...] = given_ref[...]

    half = tok_share // 2
    hist_rows = hist_ref.shape[0]
    hist_local = hist_rows // tok_share
    cand_rows = cand_ref.shape[0]
    chunk = half + CAND_HALF
    picks = [selection(owner_ref[...], member) for member in range(hist_local)]
    fill = jnp.zeros((CAND_PAD - CAND_HALF, LANES), F32)
    for pair in range(H // 2):
        lanes = slice(pair * LANES, (pair + 1) * LANES)
        cross_slab = jnp.zeros((cand_rows, LANES), F32)
        for member in range(hist_local):
            base = member * tok_share
            first = (member * H + 2 * pair) * chunk
            even = back_ref[first : first + half].astype(F32)
            odd = back_ref[first + chunk : first + chunk + half].astype(F32)
            rows_ref[base : base + half, lanes] = join(even, swap_halves(odd))
            rows_ref[base + half : base + tok_share, lanes] = join(swap_halves(even), odd)
            first = first + half
            even = back_ref[first : first + CAND_HALF].astype(F32)
            odd = back_ref[first + chunk : first + chunk + CAND_HALF].astype(F32)
            upper, lower = join(even, swap_halves(odd)), join(swap_halves(even), odd)
            found = jnp.concatenate([upper, fill, lower, fill], axis=0).astype(BF16)
            cross_slab = cross_slab + lax.dot_general(
                picks[member], found, (((0,), (0,)), ((), ())), preferred_element_type=F32
            )
        rows_ref[hist_rows:, lanes] = cross_slab
    gain = gain_ref[...]
    attended = rows_ref[...]
    scaled = rms_apply(attended, gain)
    gated = (scaled * gate_ref[...].astype(F32)).astype(BF16)
    product = jnp.dot(gated, weight_ref[...], preferred_element_type=F32)
    hist_out_ref[...] = (hist_ref[...].astype(F32) + product[:hist_rows]).astype(BF16)
    cand_out_ref[...] = (cand_ref[...].astype(F32) + product[hist_rows:]).astype(BF16)


def per_device(history, candidates, lengths, assignment, weight_in, weight_out, gain_in, gain_attn):
    seq_devices = lax.axis_size("seq")
    hist_local, tok_share, width = history.shape
    cand_count = candidates.shape[1]
    half = tok_share // 2
    hist_rows = hist_local * tok_share
    items = hist_local * H
    assert items == seq_devices
    hist = history.reshape(hist_rows, width)
    cand = candidates.reshape(cand_count, width)
    gain_in = gain_in.reshape(1, width)
    gain_attn = gain_attn.reshape(1, width)
    send_rows, back_rows = tok_share + half + CAND_HALF, half + CAND_HALF
    length = seq_devices * tok_share
    params = pltpu.CompilerParams(vmem_limit_bytes=VMEM_LIMIT)
    vmem = pl.BlockSpec(memory_space=pltpu.VMEM)

    def exchange(rows):
        pairs = rows.reshape(items, rows.shape[0] // items // 2, 2, LANES)
        moved = lax.all_to_all(pairs, "seq", split_axis=0, concat_axis=0, tiled=True)
        return pltpu.with_memory_space_constraint(moved.reshape(rows.shape), pltpu.VMEM)

    all_rows = hist_rows + cand_count
    send, normed, gate = pl.pallas_call(
        functools.partial(project_kernel, "seq", "dp", tok_share),
        in_specs=[pl.BlockSpec(memory_space=pltpu.HBM)] * 6,
        out_specs=[vmem] * 3,
        out_shape=[
            pltpu.VMEM((items * send_rows, LANES), BF16),
            pltpu.VMEM((all_rows, width), BF16),
            jax.ShapeDtypeStruct((all_rows, width), BF16),
        ],
        scratch_shapes=[
            pltpu.SMEM(lengths.shape, lengths.dtype),
            pltpu.VMEM(hist.shape, BF16),
            pltpu.VMEM(cand.shape, BF16),
            pltpu.VMEM(assignment.shape, assignment.dtype),
            pltpu.VMEM(gain_in.shape, F32),
            pltpu.VMEM((H // HEADS_STEP, PARTS, width, HEADS_STEP * HD), BF16),
            pltpu.SemaphoreType.DMA((5,)),
            pltpu.SemaphoreType.DMA((H // HEADS_STEP, PARTS)),
        ],
        compiler_params=params,
        name="project",
    )(
        *(
            pltpu.with_memory_space_constraint(argument, pltpu.HBM)
            for argument in (lengths, hist, cand, assignment, gain_in, weight_in)
        )
    )
    back = pl.pallas_call(
        functools.partial(attend_kernel, tok_share),
        in_specs=[vmem],
        out_specs=vmem,
        out_shape=pltpu.VMEM((items * back_rows, LANES), BF16),
        scratch_shapes=[
            pltpu.VMEM((length, LANES), BF16),
            pltpu.VMEM((seq_devices // GROUP, HD, GROUP * tok_share), BF16),
            pltpu.VMEM((length, LANES), BF16),
            pltpu.VMEM((seq_devices * CAP, LANES), BF16),
            pltpu.VMEM((HD, length), F32),
            pltpu.VMEM((HD, seq_devices * CAP), F32),
        ],
        compiler_params=params,
        name="attend",
    )(exchange(send))
    hist_out, cand_out = pl.pallas_call(
        functools.partial(output_kernel, "dp", tok_share),
        in_specs=[vmem] * 8 + [pl.BlockSpec(memory_space=pltpu.HBM)],
        out_specs=[vmem] * 2,
        out_shape=[
            jax.ShapeDtypeStruct((hist_rows, width), BF16),
            jax.ShapeDtypeStruct((cand_count, width), BF16),
        ],
        scratch_shapes=[
            pltpu.VMEM((all_rows, width), F32),
            pltpu.VMEM((all_rows, width), BF16),
            pltpu.VMEM((width, width), BF16),
            pltpu.SemaphoreType.DMA,
        ],
        compiler_params=params,
        name="combine",
    )(
        exchange(back),
        assignment,
        hist,
        cand,
        normed,
        gate,
        gain_attn,
        weight_out,
        pltpu.with_memory_space_constraint(weight_in, pltpu.HBM),
    )
    return hist_out.reshape(history.shape), cand_out.reshape(candidates.shape)


def solution(mesh):
    in_specs = (
        P(("groups", "dp"), "seq", None),
        P(("groups", "dp"), "seq", None),
        P(("groups", "dp")),
        P(("groups", "dp"), "seq"),
        P(),
        P(),
        P(),
        P(),
    )
    out_specs = (P(("groups", "dp"), "seq", None), P(("groups", "dp"), "seq", None))
    return jax.shard_map(
        per_device, mesh=mesh, in_specs=in_specs, out_specs=out_specs, check_vma=False
    )
```

```python
import functools

import jax
import jax.numpy as jnp
from jax import lax
from jax.experimental import pallas as pl
from jax.experimental.pallas import tpu as pltpu
from jax.sharding import PartitionSpec as P

H = 16
HD = 64
CAP = 40
LANES = 128
CAND_HALF = CAP // 2
CAND_PAD = 24
HEADS_STEP = 16
PARTS = 4
VMEM_LIMIT = 28 << 20
STAGGER_NS = 32_000
WEIGHTS_AHEAD = 2
GROUP = 8
F32 = jnp.float32
BF16 = jnp.bfloat16


def rms_apply(values, gain):
    return values * lax.rsqrt(jnp.mean(values * values, axis=-1, keepdims=True) + 1e-06) * gain


def silu(values):
    half = values * 0.5
    return half + half * jnp.tanh(half)


def swap_halves(values):
    return pltpu.roll(values, HD, 1)


def low_lanes(rows):
    return lax.broadcasted_iota(jnp.int32, (rows, LANES), 1) < HD


def join(first, second):
    return jnp.where(low_lanes(first.shape[0]), first, second)


def selection(owner_row, member):
    count = owner_row.shape[1]
    mine = (owner_row == member).astype(F32)
    before = (
        lax.broadcasted_iota(jnp.int32, (count, count), 0)
        < lax.broadcasted_iota(jnp.int32, (count, count), 1)
    ).astype(F32)
    rank = jnp.dot(jnp.broadcast_to(mine, (8, count)), before, preferred_element_type=F32)[0:1]
    row = jnp.where(rank < CAND_HALF, rank, rank + (CAND_PAD - CAND_HALF))
    row = jnp.where(mine > 0.5, row, -1.0)
    rows = lax.broadcasted_iota(jnp.int32, (2 * CAND_PAD, count), 0).astype(F32)
    return (rows == row).astype(BF16)


def project_kernel(
    axis,
    stagger_axis,
    tok_share,
    lengths_hbm,
    hist_hbm,
    cand_hbm,
    owner_hbm,
    gain_hbm,
    weight_hbm,
    send_ref,
    normed_ref,
    gate_ref,
    picks_ref,
    lengths_ref,
    hist_ref,
    cand_ref,
    owner_ref,
    gain_ref,
    weight_ref,
    loaded,
    arrived,
):
    hist_rows, width = hist_ref.shape
    hist_local = hist_rows // tok_share
    half = tok_share // 2
    chunk = tok_share + half + CAND_HALF
    step_width = HEADS_STEP * HD
    steps = H // HEADS_STEP

    def fetch(step, part):
        start = part * width + step * step_width
        return pltpu.make_async_copy(
            weight_hbm.at[:, start : start + step_width],
            weight_ref.at[step, part],
            arrived.at[step, part],
        )

    loads = [
        pltpu.make_async_copy(source, target, loaded.at[number])
        for number, (source, target) in enumerate(
            (
                (gain_hbm, gain_ref),
                (hist_hbm, hist_ref),
                (cand_hbm, cand_ref),
                (owner_hbm, owner_ref),
                (lengths_hbm, lengths_ref),
            )
        )
    ]
    for load in loads:
        load.start()
    for step in range(steps):
        for part in (2, 3, 1):
            fetch(step, part).start()
    for load in loads:
        load.wait()
    gain = gain_ref[...]
    normed_ref[:hist_rows] = rms_apply(hist_ref[...].astype(F32), gain).astype(BF16)
    normed_ref[hist_rows:] = rms_apply(cand_ref[...].astype(F32), gain).astype(BF16)
    picks = [selection(owner_ref[...], member) for member in range(hist_local)]
    for member in range(hist_local):
        picks_ref[member] = picks[member]
    position = lax.axis_index(axis) * tok_share + lax.broadcasted_iota(jnp.int32, (tok_share, LANES), 0)

    def times(step, rows, part):
        fetch(step, part).wait()
        return jnp.dot(normed_ref[:rows], weight_ref[step, part], preferred_element_type=F32)

    for step in range(steps):
        keys = times(step, hist_rows, 2)
        values = times(step, hist_rows, 3)
        query = times(step, normed_ref.shape[0], 1).astype(BF16).astype(F32) * (0.5 * HD ** (-0.5))
        cand_query = query[hist_rows:].astype(BF16)
        for member in range(hist_local):
            rows = slice(member * tok_share, (member + 1) * tok_share)
            picked = jnp.dot(picks[member], cand_query, preferred_element_type=F32)
            present = position < lengths_ref[member]
            for pair in range(HEADS_STEP // 2):
                lanes = slice(pair * LANES, (pair + 1) * LANES)
                key_slab = jnp.where(present, keys[rows, lanes], 0.0)
                value_slab, query_slab, cand_slab = values[rows, lanes], query[rows, lanes], picked[:, lanes]
                even = (member * H + step * HEADS_STEP + 2 * pair) * chunk
                odd = even + chunk
                send_ref[even : even + tok_share] = join(key_slab, swap_halves(value_slab)).astype(BF16)
                send_ref[odd : odd + tok_share] = join(swap_halves(key_slab), value_slab).astype(BF16)
                top, low = query_slab[:half], query_slab[half:]
                even, odd = even + tok_share, odd + tok_share
                send_ref[even : even + half] = join(top, swap_halves(low)).astype(BF16)
                send_ref[odd : odd + half] = join(swap_halves(top), low).astype(BF16)
                top, low = cand_slab[:CAND_PAD], cand_slab[CAND_PAD:]
                even, odd = even + half, odd + half
                send_ref[even : even + CAND_HALF] = join(top, swap_halves(low)).astype(BF16)[:CAND_HALF]
                send_ref[odd : odd + CAND_HALF] = join(swap_halves(top), low).astype(BF16)[:CAND_HALF]

    @pl.when(lax.axis_index(stagger_axis) > 0)
    def _():
        for step in range(steps):
            fetch(step, 0).start()
        for step in range(steps):
            columns = slice(step * step_width, (step + 1) * step_width)
            gate_ref[:, columns] = silu(times(step, normed_ref.shape[0], 0)).astype(BF16)
        pl.delay(STAGGER_NS)


def attend_kernel(tok_share, recv_ref, back_ref, kv_ref, vt_ref, q_ref, cq_ref, ot_ref, ct_ref):
    half = tok_share // 2
    chunk, back_chunk = tok_share + half + CAND_HALF, half + CAND_HALF
    sources = recv_ref.shape[0] // chunk
    groups = sources // GROUP
    keys_group, half_group = GROUP * tok_share, GROUP * half
    queries_group = 2 * half_group
    cands = sources * CAND_HALF

    def keys_of(group):
        return kv_ref[group * keys_group : (group + 1) * keys_group]

    def low_half(values):
        return jnp.where(low_lanes(values.shape[0]), values, 0.0).astype(BF16)

    for source in range(sources):
        base = source * chunk
        kv_ref[source * tok_share : (source + 1) * tok_share] = recv_ref[base : base + tok_share]
        base = base + tok_share
        packed = recv_ref[base : base + half].astype(F32)
        place = source // GROUP * queries_group + source % GROUP * half
        q_ref[place : place + half] = low_half(packed)
        q_ref[place + half_group : place + half_group + half] = low_half(swap_halves(packed))
        base = base + half
        packed = recv_ref[base : base + CAND_HALF].astype(F32)
        place = source * CAND_HALF
        cq_ref[place : place + CAND_HALF] = low_half(packed)
        cq_ref[cands + place : cands + place + CAND_HALF] = low_half(swap_halves(packed))
    for group in range(groups):
        vt_ref[group] = keys_of(group).T[HD:]

    column = lax.broadcasted_iota(jnp.int32, (1, queries_group), 1)
    is_low = (column >= half_group).astype(jnp.int32)
    column = column - is_low * half_group
    source = jnp.zeros_like(column)
    for later in range(1, GROUP):
        source = source + (column >= later * half).astype(jnp.int32)
    position = source * half + column + is_low * half
    causal = lax.broadcasted_iota(jnp.int32, (keys_group, queries_group), 0) <= position

    def weights(group, query, allowed):
        half_score = lax.dot_general(
            keys_of(group), query, (((1,), (1,)), ((), ())), preferred_element_type=F32
        )
        weight = half_score + half_score * jnp.tanh(half_score)
        if allowed is not None:
            weight = jnp.where(allowed, weight, 0.0)
        return weight.astype(BF16)

    def gather(ref, columns, group, weight, first):
        part = jnp.dot(vt_ref[group], weight, preferred_element_type=F32)
        ref[:, columns] = part if first else ref[:, columns] + part

    work = [(ct_ref, slice(0, 2 * cands), group, cq_ref, None, group == 0) for group in range(groups)]
    for group in range(groups):
        for after in range(group, groups):
            columns = slice(after * queries_group, (after + 1) * queries_group)
            work.append((ot_ref, columns, group, q_ref, causal if after == group else None, group == 0))
    pending = []
    for ref, columns, group, query_ref, allowed, first in work:
        pending.append((ref, columns, group, weights(group, query_ref[columns], allowed), first))
        if len(pending) > WEIGHTS_AHEAD:
            gather(*pending.pop(0))
    for waiting in pending:
        gather(*waiting)

    for group in range(groups):
        base = group * queries_group
        top = ot_ref[:, base : base + half_group]
        low = ot_ref[:, base + half_group : base + queries_group]
        joined = jnp.concatenate([top, low], axis=0).T.astype(BF16)
        for member in range(GROUP):
            place = (group * GROUP + member) * back_chunk
            back_ref[place : place + half] = joined[member * half : (member + 1) * half]
    joined = jnp.concatenate([ct_ref[:, :cands], ct_ref[:, cands:]], axis=0).T.astype(BF16)
    for source in range(sources):
        place = source * back_chunk + half
        back_ref[place : place + CAND_HALF] = joined[source * CAND_HALF : (source + 1) * CAND_HALF]


def output_kernel(
    stagger_axis,
    tok_share,
    back_ref,
    picks_ref,
    hist_ref,
    cand_ref,
    normed_ref,
    given_ref,
    gain_ref,
    weight_ref,
    weight_in_hbm,
    hist_out_ref,
    cand_out_ref,
    rows_ref,
    gate_ref,
    gate_weight_ref,
    arrived,
):
    width = hist_ref.shape[1]
    is_first = lax.axis_index(stagger_axis) == 0

    @pl.when(is_first)
    def _():
        fetch = pltpu.make_async_copy(weight_in_hbm.at[:, :width], gate_weight_ref, arrived)
        fetch.start()
        fetch.wait()
        product = jnp.dot(normed_ref[...], gate_weight_ref[...], preferred_element_type=F32)
        gate_ref[...] = silu(product).astype(BF16)

    @pl.when(jnp.logical_not(is_first))
    def _():
        gate_ref[...] = given_ref[...]

    half = tok_share // 2
    hist_rows = hist_ref.shape[0]
    hist_local = hist_rows // tok_share
    cand_rows = cand_ref.shape[0]
    chunk = half + CAND_HALF
    fill = jnp.zeros((CAND_PAD - CAND_HALF, LANES), F32)
    for pair in range(H // 2):
        lanes = slice(pair * LANES, (pair + 1) * LANES)
        cross_slab = jnp.zeros((cand_rows, LANES), F32)
        for member in range(hist_local):
            base = member * tok_share
            first = (member * H + 2 * pair) * chunk
            even = back_ref[first : first + half].astype(F32)
            odd = back_ref[first + chunk : first + chunk + half].astype(F32)
            rows_ref[base : base + half, lanes] = join(even, swap_halves(odd))
            rows_ref[base + half : base + tok_share, lanes] = join(swap_halves(even), odd)
            first = first + half
            even = back_ref[first : first + CAND_HALF].astype(F32)
            odd = back_ref[first + chunk : first + chunk + CAND_HALF].astype(F32)
            upper, lower = join(even, swap_halves(odd)), join(swap_halves(even), odd)
            found = jnp.concatenate([upper, fill, lower, fill], axis=0).astype(BF16)
            cross_slab = cross_slab + lax.dot_general(
                picks_ref[member], found, (((0,), (0,)), ((), ())), preferred_element_type=F32
            )
        rows_ref[hist_rows:, lanes] = cross_slab
    gain = gain_ref[...]
    attended = rows_ref[...]
    scaled = rms_apply(attended, gain)
    gated = (scaled * gate_ref[...].astype(F32)).astype(BF16)
    product = jnp.dot(gated, weight_ref[...], preferred_element_type=F32)
    hist_out_ref[...] = (hist_ref[...].astype(F32) + product[:hist_rows]).astype(BF16)
    cand_out_ref[...] = (cand_ref[...].astype(F32) + product[hist_rows:]).astype(BF16)


def per_device(history, candidates, lengths, assignment, weight_in, weight_out, gain_in, gain_attn):
    seq_devices = lax.axis_size("seq")
    hist_local, tok_share, width = history.shape
    cand_count = candidates.shape[1]
    half = tok_share // 2
    hist_rows = hist_local * tok_share
    items = hist_local * H
    assert items == seq_devices
    hist = history.reshape(hist_rows, width)
    cand = candidates.reshape(cand_count, width)
    gain_in = gain_in.reshape(1, width)
    gain_attn = gain_attn.reshape(1, width)
    send_rows, back_rows = tok_share + half + CAND_HALF, half + CAND_HALF
    length = seq_devices * tok_share
    params = pltpu.CompilerParams(vmem_limit_bytes=VMEM_LIMIT)
    vmem = pl.BlockSpec(memory_space=pltpu.VMEM)

    def exchange(rows):
        pairs = rows.reshape(items, rows.shape[0] // items // 2, 2, LANES)
        moved = lax.all_to_all(pairs, "seq", split_axis=0, concat_axis=0, tiled=True)
        return pltpu.with_memory_space_constraint(moved.reshape(rows.shape), pltpu.VMEM)

    all_rows = hist_rows + cand_count
    send, normed, gate, picks = pl.pallas_call(
        functools.partial(project_kernel, "seq", "dp", tok_share),
        in_specs=[pl.BlockSpec(memory_space=pltpu.HBM)] * 6,
        out_specs=[vmem] * 4,
        out_shape=[
            pltpu.VMEM((items * send_rows, LANES), BF16),
            pltpu.VMEM((all_rows, width), BF16),
            jax.ShapeDtypeStruct((all_rows, width), BF16),
            pltpu.VMEM((hist_local, 2 * CAND_PAD, cand_count), BF16),
        ],
        scratch_shapes=[
            pltpu.SMEM(lengths.shape, lengths.dtype),
            pltpu.VMEM(hist.shape, BF16),
            pltpu.VMEM(cand.shape, BF16),
            pltpu.VMEM(assignment.shape, assignment.dtype),
            pltpu.VMEM(gain_in.shape, F32),
            pltpu.VMEM((H // HEADS_STEP, PARTS, width, HEADS_STEP * HD), BF16),
            pltpu.SemaphoreType.DMA((5,)),
            pltpu.SemaphoreType.DMA((H // HEADS_STEP, PARTS)),
        ],
        compiler_params=params,
        name="project",
    )(
        *(
            pltpu.with_memory_space_constraint(argument, pltpu.HBM)
            for argument in (lengths, hist, cand, assignment, gain_in, weight_in)
        )
    )
    back = pl.pallas_call(
        functools.partial(attend_kernel, tok_share),
        in_specs=[vmem],
        out_specs=vmem,
        out_shape=pltpu.VMEM((items * back_rows, LANES), BF16),
        scratch_shapes=[
            pltpu.VMEM((length, LANES), BF16),
            pltpu.VMEM((seq_devices // GROUP, HD, GROUP * tok_share), BF16),
            pltpu.VMEM((length, LANES), BF16),
            pltpu.VMEM((seq_devices * CAP, LANES), BF16),
            pltpu.VMEM((HD, length), F32),
            pltpu.VMEM((HD, seq_devices * CAP), F32),
        ],
        compiler_params=params,
        name="attend",
    )(exchange(send))
    hist_out, cand_out = pl.pallas_call(
        functools.partial(output_kernel, "dp", tok_share),
        in_specs=[vmem] * 8 + [pl.BlockSpec(memory_space=pltpu.HBM)],
        out_specs=[vmem] * 2,
        out_shape=[
            jax.ShapeDtypeStruct((hist_rows, width), BF16),
            jax.ShapeDtypeStruct((cand_count, width), BF16),
        ],
        scratch_shapes=[
            pltpu.VMEM((all_rows, width), F32),
            pltpu.VMEM((all_rows, width), BF16),
            pltpu.VMEM((width, width), BF16),
            pltpu.SemaphoreType.DMA,
        ],
        compiler_params=params,
        name="combine",
    )(
        exchange(back),
        picks,
        hist,
        cand,
        normed,
        gate,
        gain_attn,
        weight_out,
        pltpu.with_memory_space_constraint(weight_in, pltpu.HBM),
    )
    return hist_out.reshape(history.shape), cand_out.reshape(candidates.shape)


def solution(mesh):
    in_specs = (
        P(("groups", "dp"), "seq", None),
        P(("groups", "dp"), "seq", None),
        P(("groups", "dp")),
        P(("groups", "dp"), "seq"),
        P(),
        P(),
        P(),
        P(),
    )
    out_specs = (P(("groups", "dp"), "seq", None), P(("groups", "dp"), "seq", None))
    return jax.shard_map(
        per_device, mesh=mesh, in_specs=in_specs, out_specs=out_specs, check_vma=False
    )
```
